256 devices in a mesh: section: 8 (over x, z_lo), dp: 32 (over y, z_hi, core).
Axes of the slice: x: 4, y: 4, z: 8 (z_hi: 4, z_lo: 2; z = z_hi * 2 + z_lo), core: 2. Of those that a mesh axis runs over, the one named last changes fastest.
Arguments:
- activations: bfloat16 [64, 512, 4608], P('section', 'dp'), may hold values from -6 to 6
- section_sources: int32 [64], replicated, may hold values from 0 to 63, as said below
- accumulators: float32 [1024, 16, 4608], P('dp', 'section'), may hold values from -6 to 6
- block_sources: int32 [1024], replicated, may hold values from 0 to 1023, as said below
- loss_terms: float32 [8, 32], P('section', 'dp'), may hold values from 0.35 to 6
- pre_gain: float32 [8, 4608], P('section'), may hold values from 0.1 to 1.9
- query_weight: bfloat16 [8, 4608, 4096], P('section', None, 'dp'), may hold values from -0.09375 to 0.09375
- keyval_weight: bfloat16 [8, 4608, 4096], P('section', None, 'dp'), may hold values from -0.09375 to 0.09375
- output_weight: bfloat16 [8, 4096, 4608], P('section', 'dp'), may hold values from -0.09375 to 0.09375
- post_gain: float32 [8, 4608], P('section'), may hold values from 0.1 to 1.9
Outputs:
- new_activations: bfloat16 [64, 512, 4608], P('section', 'dp')
- new_accumulators: float32 [1024, 16, 4608], P('dp', 'section')
- check_out: bfloat16 [8, 512, 4608], P('section', 'dp')
The draws below stay inside these ranges and needn't reach their ends.
Inputs may be any that keep to these rules, and one draw needn't show every extreme that they name: `section_sources`: A permutation; each old section's micro-batches fill 1 slots of each new section. `block_sources`: A permutation; each old data index's blocks fill 1 block of each new data index.
All inputs are finite; a program needn't handle non-finite values.
Results may differ from the reference program's by a relative error of at most 0.014.
Values may be sent and summed in bfloat16 or wider, within the bound.
A program may use at most 64 MiB of HBM per device.

```python
import jax
import jax.numpy as jnp
from jax import lax

D = 4608
HD = 128
HEADS = 32
KV_HEADS = 16
TOKENS = 512
MB_DEV = 8
MB_ALL = 64
BROWS = 2
BLK_DEV = 32
BLOCKS = 1024
ACC_ROWS = 16
N_SECTION = 8
N_DP = 32


def balanced_sources(key, groups, per_group):
    per_peer = per_group // groups

    def source_order(which):
        return jax.random.permutation(jax.random.fold_in(key, which), per_group)
    orders = jax.vmap(source_order)(jnp.arange(groups, dtype=jnp.int32))
    sources = jnp.arange(groups, dtype=jnp.int32)[:, None] * per_group + orders.astype(jnp.int32)
    chosen = sources.reshape(groups, groups, per_peer).transpose(1, 0, 2).reshape(groups, per_group)

    def shuffle(which, entries):
        return jax.random.permutation(jax.random.fold_in(key, 100000 + which), entries)
    table = jax.vmap(shuffle)(jnp.arange(groups, dtype=jnp.int32), chosen)
    return table.reshape(-1).astype(jnp.int32)


def draw_section_sources(key, part):
    return balanced_sources(jax.random.fold_in(key, 11), N_SECTION, MB_DEV)


def draw_block_sources(key, part):
    return balanced_sources(jax.random.fold_in(key, 23), N_DP, BLK_DEV)


def draw_loss_terms(key, part):
    rising = 1.0 + 2.0 * jnp.arange(N_DP, dtype=jnp.float32) / (N_DP - 1)
    subkey = jax.random.fold_in(key, 37)
    factor = jnp.exp(jax.random.uniform(subkey, (N_SECTION, N_DP), jnp.float32, jnp.log(0.7), jnp.log(1.4)))
    return (rising[None, :] * factor).astype(jnp.float32)


def shard_levels(stream_key, extent, shards, smallest, top_value):
    loudness, own = 1.0, jax.random.fold_in(stream_key, 6)
    for axis_at, blocks in shards:
        steps = jnp.exp(jax.random.uniform(jax.random.fold_in(own, axis_at), (blocks,), jnp.float32, smallest / len(shards), top_value / len(shards)))
        loudness = loudness * jnp.repeat(steps, extent[axis_at] // blocks).reshape([-1 if axis == axis_at else 1 for axis in range(len(extent))])
    return loudness


def bell_draw(rng, extent, spread, reach, shards=(), held_as=jnp.bfloat16):
    values = jax.random.normal(rng, extent, jnp.float32) * spread
    if len(shards) > 0:
        values = shard_levels(rng, extent, shards, -0.22, 0.18) * values
    return jnp.clip(values, min=-reach, max=reach).astype(held_as)


def setup_inputs(seed: int = 0) -> dict:
    seeds = jax.random.split(jax.random.key(seed), 11)
    activations = bell_draw(seeds[0], (MB_ALL, TOKENS, D), 1.0, 6.0, ((0, 8), (1, 32)))
    section_sources = draw_section_sources(jax.random.fold_in(seeds[10], 71), 0)
    accumulators = bell_draw(seeds[2], (BLOCKS, ACC_ROWS, D), 1.0, 6.0, ((0, 32), (1, 8)), jnp.float32)
    block_sources = draw_block_sources(jax.random.fold_in(seeds[10], 71), 0)
    loss_terms = draw_loss_terms(jax.random.fold_in(seeds[10], 71), 0)
    pre_gain = jnp.clip(1.0 + 0.18 * jax.random.normal(seeds[5], (N_SECTION, D), jnp.float32), 0.1, 1.9)
    query_weight = bell_draw(seeds[6], (N_SECTION, D, HEADS * HD), D ** -0.5, 0.09375, ((0, 8), (2, 32)))
    keyval_weight = bell_draw(seeds[7], (N_SECTION, D, HEADS * HD), D ** -0.5, 0.09375, ((0, 8), (2, 32)))
    output_weight = bell_draw(seeds[8], (N_SECTION, HEADS * HD, D), (HEADS * HD) ** -0.5, 0.09375, ((0, 8), (1, 32)))
    post_gain = jnp.clip(1.0 + 0.18 * jax.random.normal(seeds[9], (N_SECTION, D), jnp.float32), 0.1, 1.9)
    return dict(activations=activations, section_sources=section_sources, accumulators=accumulators, block_sources=block_sources, loss_terms=loss_terms, pre_gain=pre_gain, query_weight=query_weight, keyval_weight=keyval_weight, output_weight=output_weight, post_gain=post_gain)


def rms_norm(values, gain):
    meansq = lax.optimization_barrier(jnp.mean(values * values, axis=-1, keepdims=True))
    return values * lax.rsqrt(meansq + 1e-06) * gain

def rotary(values, positions):
    width = values.shape[-1]
    middle = width // 2
    counter = jnp.arange(middle, dtype=jnp.float32)
    freqs = 10000.0 ** (-2.0 * counter / width)
    angles = positions.astype(jnp.float32)[:, None] * freqs[None, :]
    cosine = jnp.cos(angles)
    sine = jnp.sin(angles)
    if values.ndim == 3:
        cosine = cosine[:, None, :]
        sine = sine[:, None, :]
    first = values[..., :middle]
    second = values[..., middle:]
    return jnp.concatenate([first * cosine - second * sine, second * cosine + first * sine], axis=-1)

def check_layer(checked, gain_pre, w_query, w_keyval, w_output, gain_post):
    length = checked.shape[0]
    positions = jnp.arange(length, dtype=jnp.int32)
    normed = rms_norm(checked.astype(jnp.float32), gain_pre).astype(jnp.bfloat16)
    queries = jnp.dot(normed, w_query, preferred_element_type=jnp.float32).reshape(length, HEADS, HD)
    keyvals = jnp.dot(normed, w_keyval, preferred_element_type=jnp.float32).reshape(length, KV_HEADS, 2, HD)
    queries = rotary(queries, positions).astype(jnp.bfloat16)
    key_rows = rotary(keyvals[:, :, 0, :], positions).astype(jnp.bfloat16)
    value_rows = keyvals[:, :, 1, :].astype(jnp.bfloat16)
    key_rows = jnp.repeat(key_rows, 2, axis=1)
    value_rows = jnp.repeat(value_rows, 2, axis=1)
    scale_factor = (D / HEADS) ** (-0.5)
    scores = jnp.einsum('qhd,khd->hqk', queries.astype(jnp.float32), key_rows.astype(jnp.float32)) * scale_factor
    capped = 50.0 * jnp.tanh(scores / 50.0)
    causal = positions[None, :] <= positions[:, None]
    expd = jnp.where(causal[None, :, :], jnp.exp(capped), 0.0)
    denominator = lax.optimization_barrier(jnp.sum(expd, axis=-1))
    probs = expd.astype(jnp.bfloat16)
    numer = jnp.einsum('hqk,khd->hqd', probs.astype(jnp.float32), value_rows.astype(jnp.float32))
    attended = (numer / denominator[:, :, None]).astype(jnp.bfloat16)
    attended = jnp.transpose(attended, (1, 0, 2)).reshape(length, HEADS * HD)
    summed = jnp.dot(attended, w_output, preferred_element_type=jnp.float32)
    return (checked.astype(jnp.float32) + rms_norm(summed, gain_post)).astype(jnp.bfloat16)

def reference(activations, section_sources, accumulators, block_sources, loss_terms, pre_gain, query_weight, keyval_weight, output_weight, post_gain):
    moved = jnp.take(activations, section_sources, axis=0)
    regrouped = jnp.take(accumulators, block_sources, axis=0)
    totals = lax.optimization_barrier(jnp.sum(loss_terms, axis=1))
    factor = N_DP / totals
    scaled = regrouped.reshape(BLOCKS, N_SECTION, BROWS, D) * factor[None, :, None, None]
    new_accumulators = scaled.reshape(BLOCKS, ACC_ROWS, D)
    checks = []
    for section_id in range(N_SECTION):
        checks.append(check_layer(moved[section_id * MB_DEV], pre_gain[section_id], query_weight[section_id], keyval_weight[section_id], output_weight[section_id], post_gain[section_id]))
    return (moved, new_accumulators, jnp.stack(checks, axis=0))
```

```python
import functools

import jax
import jax.numpy as jnp
import numpy as np
from jax import lax
from jax.experimental import pallas as pl
from jax.experimental.pallas import tpu as pltpu
from jax.sharding import PartitionSpec as P

MESH = pl.DeviceIdType.MESH
D = 4608
H = D // 2
HD = 128
NS = 8
NY = 4
NZ = 4
MB = 8
ROWS = 16
BLK = 32
EPS = 1e-06
F32 = jnp.float32
BF16 = jnp.bfloat16


def rotary_tables():
    freqs = (10000.0 ** (-2.0 * np.arange(HD // 2, dtype=np.float32) / HD)).astype(np.float32)
    angles = np.arange(512, dtype=np.float32)[:, None] * freqs[None, :]
    cosine, sine = np.cos(angles), np.sin(angles)
    full = np.stack(
        [np.concatenate([cosine, cosine], axis=1), np.concatenate([-sine, sine], axis=1)]
    )
    return full.astype(np.float32).reshape(2, NY, NZ, 32, HD)


def kernel(
    sec, blk, act_hbm, acc_hbm, loss_ref, gpre, wq_hbm, wkv_hbm, wo_hbm, gpost, tab,
    moved_hbm, newacc_hbm, check_hbm,
    act_v, asend, recv_a, moved_v, acc_v, bsend, b1, b2, b3, newacc_v,
    lsend, lry, lsum, lrz, lfin, lrc,
    nbuf, xh, wbuf, wobuf, rbuf, rrq, rrkv, qf, kf, vf, at2,
    pbuf, yrh, yrf, zrh, zrf, zs, fb, finr, outb, checkb,
    loc, a_s, a_r, bl_s, bl_r, cz_s, cz_r, cy_s, cy_r, cc_s, cc_r, dy_s, dy_r, dz_s, dz_r,
):
    s = lax.axis_index("section")
    d = lax.axis_index("dp")
    y = lax.div(d, 8)
    z = lax.rem(lax.div(d, 2), 4)
    c = lax.rem(d, 2)
    o = 1 - c

    def ring(v, r, n):
        return lax.rem(v + (r + n), n)

    def dp_of(yy, zz, cc):
        return (yy * NZ + zz) * 2 + cc

    at_y = {r: (s, dp_of(ring(y, r, NY), z, c)) for r in (1, 2, 3, -1)}
    at_z = {r: (s, dp_of(y, ring(z, r, NZ), c)) for r in (1, 2, 3, -1)}
    at_c = (s, dp_of(y, z, o))
    at_s = {r: (ring(s, r, NS), d) for r in range(1, NS)}

    barrier = pltpu.get_barrier_semaphore()
    greet = [at_s[r] for r in range(1, NS)] + [at_y[r] for r in (1, 2, 3)]
    greet += [at_z[r] for r in (1, 2, 3)] + [at_c]
    for who in greet:
        pl.semaphore_signal(barrier, inc=1, device_id=who, device_id_type=MESH)

    pending = []

    def remote(src, dst, send_sem, recv_sem, who):
        copy = pltpu.make_async_remote_copy(
            src_ref=src, dst_ref=dst, send_sem=send_sem, recv_sem=recv_sem,
            device_id=who, device_id_type=MESH,
        )
        copy.start()
        pending.append(copy)
        return copy

    load_act = pltpu.make_async_copy(act_hbm, act_v, loc.at[0])
    load_acc = pltpu.make_async_copy(acc_hbm, acc_v, loc.at[1])
    own_rows = pl.ds(pl.multiple_of(c * H, 128), H)
    own_lanes = pl.ds(pl.multiple_of(c * HD, 128), HD)
    kv_lanes = pl.ds(pl.multiple_of(2 * HD + c * HD, 128), HD)
    other_rows = pl.ds(pl.multiple_of(o * H, 128), H)
    load_wq = pltpu.make_async_copy(wq_hbm.at[own_rows, :], wbuf.at[:, own_lanes], loc.at[2])
    load_wkv = pltpu.make_async_copy(wkv_hbm.at[own_rows, :], wbuf.at[:, kv_lanes], loc.at[3])
    load_wo = pltpu.make_async_copy(wo_hbm.at[:, own_rows], wobuf.at[c], loc.at[4])
    load_act.start()
    load_acc.start()
    load_wq.start()
    load_wkv.start()
    load_wo.start()

    load_act.wait()
    for r in range(NS):
        to = ring(s, r, NS)
        at = jnp.int32(0)
        for j in range(MB):
            source = sec[to * MB + j]
            at = at + jnp.where((source >> 3) == s, source & 7, 0)
        if r == 0:
            recv_a[s] = act_v[at]
        else:
            asend[r] = act_v[at]
    lsend[...] = jnp.broadcast_to(loss_ref[...], (1, HD))

    pl.semaphore_wait(barrier, len(greet))

    from_s = [
        remote(asend.at[r], recv_a.at[s], a_s.at[r], a_r.at[r], at_s[r]) for r in range(1, NS)
    ]
    from_ly = [
        remote(lsend, lry.at[r], bl_s.at[8 + r], bl_r.at[8 + r], at_y[r]) for r in (1, 2, 3)
    ]
    w_q = remote(wq_hbm.at[other_rows, :], wbuf.at[:, own_lanes], cc_s.at[0], cc_r.at[0], at_c)
    w_kv = remote(wkv_hbm.at[other_rows, :], wbuf.at[:, kv_lanes], cc_s.at[1], cc_r.at[1], at_c)
    w_o = remote(wo_hbm.at[:, other_rows], wobuf.at[c], cc_s.at[2], cc_r.at[2], at_c)

    load_acc.wait()
    from_by = []
    for r in (1, 2, 3, 0):
        base = ring(y, r, NY) * 8

        def pick(k, carry, r=r, base=base):
            first = (base + k) * BLK
            at = jnp.int32(0)
            for b in range(BLK):
                source = blk[first + b]
                at = at + jnp.where((source >> 5) == d, source & 31, 0)
            into = b1.at[0] if r == 0 else bsend.at[r]
            into[lax.div(k, 2), lax.rem(k, 2)] = acc_v[at].astype(BF16)
            return carry

        lax.fori_loop(0, 8, pick, 0)
        if r:
            from_by.append(
                remote(bsend.at[r], b1.at[r], bl_s.at[r], bl_r.at[r], at_y[r])
            )

    for copy in from_s:
        copy.wait_recv()
    x = recv_a[sec[s * MB] >> 3]
    xf = x.astype(F32)
    meansq = jnp.mean(xf * xf, axis=-1, keepdims=True)
    normed = (xf * lax.rsqrt(meansq + EPS) * gpre[...]).astype(BF16)
    nbuf[0] = normed[:, :H]
    nbuf[1] = normed[:, H:]
    xh[y, z, c] = nbuf[c]
    core_n = remote(nbuf.at[o], xh.at[y, z, c], cc_s.at[3], cc_r.at[3], at_c)
    core_n.wait_recv()

    def gather_y(q, zz):
        return [
            remote(xh.at[y, zz], xh.at[y, zz], cy_s.at[q, 0], cy_r.at[q, 0], at_y[1]),
            remote(xh.at[y, zz], xh.at[y, zz], cy_s.at[q, 1], cy_r.at[q, 1], at_y[-1]),
        ]

    def pass_y(q, zz, copies):
        copies[0].wait_recv()
        low = xh.at[ring(y, -1, NY), zz, 0]
        first = remote(low, low, cy_s.at[q, 2], cy_r.at[q, 2], at_y[1])
        copies[1].wait_recv()
        high = xh.at[ring(y, 1, NY), zz, 1]
        return [first, remote(high, high, cy_s.at[q, 3], cy_r.at[q, 3], at_y[-1])]

    zp, zm, zf = ring(z, 1, NZ), ring(z, -1, NZ), ring(z, 2, NZ)
    order = [z, zm, zp, zf]
    near_z = [
        remote(xh.at[y, z], xh.at[y, z], cz_s.at[0], cz_r.at[0], at_z[1]),
        remote(xh.at[y, z], xh.at[y, z], cz_s.at[1], cz_r.at[1], at_z[-1]),
    ]
    near = [gather_y(0, z)]
    far = [pass_y(0, z, near[0])]
    near_z[0].wait_recv()
    far_z = [remote(xh.at[y, zm, 0], xh.at[y, zm, 0], cz_s.at[2], cz_r.at[2], at_z[1])]
    near.append(gather_y(1, zm))
    near_z[1].wait_recv()
    far_z.append(remote(xh.at[y, zp, 1], xh.at[y, zp, 1], cz_s.at[3], cz_r.at[3], at_z[-1]))
    near.append(gather_y(2, zp))

    for copy in from_ly:
        copy.wait_recv()
    lsum[...] = lsend[...] + lry[1] + lry[2] + lry[3]
    from_lz = [
        remote(lsum, lrz.at[r], bl_s.at[11 + r], bl_r.at[11 + r], at_z[r]) for r in (1, 2, 3)
    ]
    for copy in from_by:
        copy.wait_recv()
    from_bz = [
        remote(b1.at[:, ring(z, r, NZ)], b2.at[r], bl_s.at[3 + r], bl_r.at[3 + r], at_z[r])
        for r in (1, 2, 3)
    ]
    b2[0] = b1[:, z]

    far.append(pass_y(1, zm, near[1]))

    def project(q):
        zz = order[q]
        for copy in far[q]:
            copy.wait_recv()
        rows = xh[:, zz].reshape(128, H)
        res = jnp.dot(rows, wbuf[...], preferred_element_type=F32)
        for j in range(4):
            rbuf[q, j] = res[:, j * HD : (j + 1) * HD]
        return [
            remote(rbuf.at[q, o], rrq.at[q], cc_s.at[4 + q], cc_r.at[4 + q], at_c),
            remote(rbuf.at[q, pl.ds(2, 2)], rrkv.at[q], cc_s.at[8 + q], cc_r.at[8 + q], at_c),
        ]

    def finish(q, copies):
        zz = order[q]
        for copy in copies:
            copy.wait_recv()
        cosine = tab[0, :, zz].reshape(128, HD)
        sine = tab[1, :, zz].reshape(128, HD)
        query = rbuf[q, c] + rrq[q]
        key = rbuf[q, 2] + rrkv[q, 0]
        value = rbuf[q, 3] + rrkv[q, 1]
        query = query * cosine + pltpu.roll(query, HD // 2, 1) * sine
        key = key * cosine + pltpu.roll(key, HD // 2, 1) * sine
        qf[:, zz] = query.astype(BF16).reshape(NY, 32, HD)
        kf[:, zz] = key.astype(BF16).reshape(NY, 32, HD)
        vf[:, zz] = value.astype(BF16).reshape(NY, 32, HD)

    load_wq.wait()
    load_wkv.wait()
    w_q.wait_recv()
    w_kv.wait_recv()
    shared = [project(0)]
    for copy in far_z:
        copy.wait_recv()
    near.append(gather_y(3, zf))
    far.append(pass_y(2, zp, near[2]))
    for j in range(MB):
        moved_v[j] = recv_a[sec[s * MB + j] >> 3]
    store_moved = pltpu.make_async_copy(moved_v, moved_hbm, loc.at[5])
    store_moved.start()
    shared.append(project(1))
    finish(0, shared[0])
    far.append(pass_y(3, zf, near[3]))
    shared.append(project(2))
    finish(1, shared[1])
    shared.append(project(3))
    finish(2, shared[2])
    finish(3, shared[3])

    from_att = []
    for m in range(NY):
        keys = 128 * (m + 1)
        scores = lax.dot_general(
            qf[m].reshape(128, HD), kf[0 : m + 1].reshape(keys, HD),
            (((1,), (1,)), ((), ())), preferred_element_type=F32,
        ) * ((D / 32) ** (-0.5))
        capped = 50.0 * jnp.tanh(scores / 50.0)
        row = lax.broadcasted_iota(jnp.int32, (128, keys), 0) + 128 * m
        col = lax.broadcasted_iota(jnp.int32, (128, keys), 1)
        expd = jnp.where(col <= row, jnp.exp(capped), 0.0)
        total = jnp.sum(expd, axis=-1, keepdims=True)
        numer = jnp.dot(
            expd.astype(BF16), vf[0 : m + 1].reshape(keys, HD), preferred_element_type=F32
        )
        at2[c, m] = (numer / total).astype(BF16).reshape(NZ, 32, HD)
        from_att.append(
            remote(at2.at[c, m], at2.at[c, m], cc_s.at[12 + m], cc_r.at[12 + m], at_c)
        )

    load_wo.wait()
    w_o.wait_recv()
    for copy in from_att:
        copy.wait_recv()
    y1, y3, y2 = ring(y, 1, NY), ring(y, -1, NY), ring(y, 2, NY)
    back = [zf, zp, zm, z]
    halves, fulls = [], []

    def part(q):
        zz = back[q]
        first = at2[0, :, zz].reshape(128, HD)
        second = at2[1, :, zz].reshape(128, HD)
        res = jnp.dot(first, wobuf[0], preferred_element_type=F32)
        res = res + jnp.dot(second, wobuf[1], preferred_element_type=F32)
        pbuf[:, zz] = res.astype(BF16).reshape(NY, 2, ROWS, H)
        halves.append([
            remote(pbuf.at[y2, zz, 0], yrh.at[q, 0], dy_s.at[q, 0], dy_r.at[q, 0], at_y[1]),
            remote(pbuf.at[y2, zz, 1], yrh.at[q, 1], dy_s.at[q, 1], dy_r.at[q, 1], at_y[-1]),
        ])

    def middle(q):
        zz = back[q]
        halves[q][0].wait_recv()
        pbuf[y1, zz, 0] = (pbuf[y1, zz, 0].astype(F32) + yrh[q, 0].astype(F32)).astype(BF16)
        up = remote(pbuf.at[y1, zz], yrf.at[q, 0], dy_s.at[q, 2], dy_r.at[q, 2], at_y[1])
        halves[q][1].wait_recv()
        pbuf[y3, zz, 1] = (pbuf[y3, zz, 1].astype(F32) + yrh[q, 1].astype(F32)).astype(BF16)
        down = remote(pbuf.at[y3, zz], yrf.at[q, 1], dy_s.at[q, 3], dy_r.at[q, 3], at_y[-1])
        fulls.append([up, down])

    def reduced(q):
        for copy in fulls[q]:
            copy.wait_recv()
        return pbuf[y, back[q]].astype(F32) + yrf[q, 0].astype(F32) + yrf[q, 1].astype(F32)

    part(0)
    part(1)
    middle(0)
    part(2)
    middle(1)
    part(3)
    zs[0] = reduced(0).astype(BF16)
    z_half = [
        remote(zs.at[0, 0], zrh.at[0], dz_s.at[0], dz_r.at[0], at_z[1]),
        remote(zs.at[0, 1], zrh.at[1], dz_s.at[1], dz_r.at[1], at_z[-1]),
    ]
    middle(2)
    middle(3)

    for copy in from_bz + from_lz:
        copy.wait_recv()
    core_b = remote(b2.at[:, :, o], b3, bl_s.at[7], bl_r.at[7], at_c)
    lfin[...] = lsum[...] + lrz[1] + lrz[2] + lrz[3]
    core_l = remote(lfin, lrc, bl_s.at[15], bl_r.at[15], at_c)

    part_sum = reduced(1)
    z_half[0].wait_recv()
    zs[1, 0] = (part_sum[0] + zrh[0].astype(F32)).astype(BF16)
    zs[1, 1] = part_sum[1].astype(BF16)
    z_up = remote(zs.at[1], zrf.at[0], dz_s.at[2], dz_r.at[2], at_z[1])
    part_sum = reduced(2)
    z_half[1].wait_recv()
    zs[2, 0] = part_sum[0].astype(BF16)
    zs[2, 1] = (part_sum[1] + zrh[1].astype(F32)).astype(BF16)
    z_down = remote(zs.at[2], zrf.at[1], dz_s.at[3], dz_r.at[3], at_z[-1])

    core_l.wait_recv()
    core_b.wait_recv()
    factor = 32.0 / (lfin[...] + lrc[...])

    def place(b, carry):
        source = blk[d * BLK + b] >> 5
        ry = (y - (source >> 3)) & 3
        rz = (z - ((source >> 1) & 3)) & 3
        mine = b2[rz, ry, c].astype(F32)
        theirs = b3[rz, ry].astype(F32)
        newacc_v[b] = jnp.where((source & 1) == c, mine, theirs) * factor
        return carry

    lax.fori_loop(0, BLK, place, 0)
    store_acc = pltpu.make_async_copy(newacc_v, newacc_hbm, loc.at[6])
    store_acc.start()

    part_sum = reduced(3)
    z_up.wait_recv()
    z_down.wait_recv()
    fb[...] = part_sum + zrf[0].astype(F32) + zrf[1].astype(F32)
    last = remote(fb.at[o], finr, cc_s.at[16], cc_r.at[16], at_c)
    checked = recv_a[sec[s * MB] >> 3].astype(F32)
    last.wait_recv()
    mine = fb[c]
    theirs = finr[...]
    meansq = jnp.sum(mine * mine, axis=-1, keepdims=True)
    meansq = (meansq + jnp.sum(theirs * theirs, axis=-1, keepdims=True)) / D
    scale = lax.rsqrt(meansq + EPS)
    outb[c] = mine
    outb[o] = theirs
    for h in range(2):
        cols = slice(h * H, (h + 1) * H)
        checkb[h] = (checked[:, cols] + outb[h] * scale * gpost[:, cols]).astype(BF16)
    stores = [
        pltpu.make_async_copy(checkb.at[h], check_hbm.at[:, pl.ds(h * H, H)], loc.at[7 + h])
        for h in range(2)
    ]
    for copy in stores:
        copy.start()
    for copy in pending:
        copy.wait_send()
    for copy in [store_moved, store_acc] + stores:
        copy.wait()


def on_device(act, sec, acc, blk, loss, gpre, wq, wkv, wo, gpost):
    acc = acc.reshape(BLK, 2, D // HD, HD).transpose(0, 2, 1, 3).reshape(BLK, 72, HD)
    tab = jnp.asarray(rotary_tables())
    any_ = pl.BlockSpec(memory_space=pl.ANY)
    smem = pl.BlockSpec(memory_space=pltpu.SMEM)
    vmem = pl.BlockSpec(memory_space=pltpu.VMEM)
    V = pltpu.VMEM
    dma = pltpu.SemaphoreType.DMA
    moved, newacc, check = pl.pallas_call(
        kernel,
        out_shape=(
            jax.ShapeDtypeStruct((MB, ROWS, D), BF16),
            jax.ShapeDtypeStruct((BLK, 72, HD), F32),
            jax.ShapeDtypeStruct((ROWS, D), BF16),
        ),
        in_specs=[smem, smem, any_, any_, vmem, vmem, any_, any_, any_, vmem, vmem],
        out_specs=(any_, any_, any_),
        scratch_shapes=[
            V((MB, ROWS, D), BF16), V((NS, ROWS, D), BF16), V((NS, ROWS, D), BF16),
            V((MB, ROWS, D), BF16), V((BLK, 72, HD), F32),
            V((NY, NZ, 2, 72, HD), BF16), V((NY, NZ, 2, 72, HD), BF16),
            V((NZ, NY, 2, 72, HD), BF16), V((NZ, NY, 72, HD), BF16), V((BLK, 72, HD), F32),
            V((1, HD), F32), V((4, 1, HD), F32), V((1, HD), F32), V((4, 1, HD), F32),
            V((1, HD), F32), V((1, HD), F32),
            V((2, ROWS, H), BF16), V((NY, NZ, 2, ROWS, H), BF16), V((H, 4 * HD), BF16),
            V((2, HD, H), BF16), V((4, 4, 128, HD), F32), V((4, 128, HD), F32),
            V((4, 2, 128, HD), F32), V((NY, NZ, 32, HD), BF16), V((NY, NZ, 32, HD), BF16),
            V((NY, NZ, 32, HD), BF16), V((2, NY, NZ, 32, HD), BF16),
            V((NY, NZ, 2, ROWS, H), BF16), V((4, 2, ROWS, H), BF16),
            V((4, 2, 2, ROWS, H), BF16), V((2, ROWS, H), BF16), V((2, 2, ROWS, H), BF16),
            V((3, 2, ROWS, H), BF16), V((2, ROWS, H), F32), V((ROWS, H), F32),
            V((2, ROWS, H), F32), V((2, ROWS, H), BF16),
            dma((9,)), dma((NS,)), dma((NS,)), dma((16,)), dma((16,)), dma((4,)), dma((4,)),
            dma((4, 4)), dma((4, 4)), dma((17,)), dma((17,)), dma((4, 4)), dma((4, 4)),
            dma((4,)), dma((4,)),
        ],
        compiler_params=pltpu.CompilerParams(
            collective_id=0, has_side_effects=True, vmem_limit_bytes=60 * 1024 * 1024
        ),
        name="restore",
    )(sec, blk, act, acc, loss, gpre, wq[0], wkv[0], wo[0], gpost, tab)
    newacc = newacc.reshape(BLK, D // HD, 2, HD).transpose(0, 2, 1, 3).reshape(BLK, 2, D)
    return moved, newacc, check[None]


def solution(mesh):
    placed = (
        P("section", "dp", None),
        P(),
        P("dp", "section", None),
        P(),
        P("section", "dp"),
        P("section", None),
        P("section", None, "dp"),
        P("section", None, "dp"),
        P("section", "dp", None),
        P("section", None),
    )
    return jax.shard_map(
        on_device,
        mesh=mesh,
        in_specs=placed,
        out_specs=(P("section", "dp", None), P("dp", "section", None), P("section", "dp", None)),
        check_vma=False,
    )
```

```python
import functools

import jax
import jax.numpy as jnp
import numpy as np
from jax import lax
from jax.experimental import pallas as pl
from jax.experimental.pallas import tpu as pltpu
from jax.sharding import PartitionSpec as P

MESH = pl.DeviceIdType.MESH
D = 4608
H = D // 2
HD = 128
NS = 8
NY = 4
NZ = 4
MB = 8
ROWS = 16
BLK = 32
EPS = 1e-06
F32 = jnp.float32
BF16 = jnp.bfloat16


def rotary_tables():
    freqs = (10000.0 ** (-2.0 * np.arange(HD // 2, dtype=np.float32) / HD)).astype(np.float32)
    angles = np.arange(512, dtype=np.float32)[:, None] * freqs[None, :]
    cosine, sine = np.cos(angles), np.sin(angles)
    full = np.stack(
        [np.concatenate([cosine, cosine], axis=1), np.concatenate([-sine, sine], axis=1)]
    )
    return full.astype(np.float32).reshape(2, NY, NZ, 32, HD)


def kernel(
    sec, blk, act_hbm, acc_hbm, loss_ref, gpre, wq_hbm, wkv_hbm, wo_hbm, gpost, tab,
    moved_hbm, newacc_hbm, check_hbm,
    act_v, asend, recv_a, moved_v, acc_v, bsend, b1, b2, b3, bre, newacc_v,
    lsend, lry, lsum, lrz, lfin, lrc,
    nbuf, xh, wbuf, wobuf, rbuf, rrq, rrkv, qf, kf, vf, at2,
    pbuf, yrh, yro, yrm, zrh, zro, zrm, zs, fb, finr, outb, checkb,
    loc, a_s, a_r, bl_s, bl_r, cz_s, cz_r, cy_s, cy_r, cc_s, cc_r, dy_s, dy_r, dz_s, dz_r, bz_s, bz_r,
):
    s = lax.axis_index("section")
    d = lax.axis_index("dp")
    y = lax.div(d, 8)
    z = lax.rem(lax.div(d, 2), 4)
    c = lax.rem(d, 2)
    o = 1 - c

    def ring(v, r, n):
        return lax.rem(v + (r + n), n)

    def dp_of(yy, zz, cc):
        return (yy * NZ + zz) * 2 + cc

    at_y = {r: (s, dp_of(ring(y, r, NY), z, c)) for r in (1, 2, 3, -1)}
    at_z = {r: (s, dp_of(y, ring(z, r, NZ), c)) for r in (1, 2, 3, -1)}
    at_c = (s, dp_of(y, z, o))
    ahead = 1 - 2 * c
    ya, yb, yf = ring(y, ahead, NY), ring(y, -ahead, NY), ring(y, 2, NY)
    za, zb, zf = ring(z, ahead, NZ), ring(z, -ahead, NZ), ring(z, 2, NZ)
    to_ya, to_yb = (s, dp_of(ya, z, c)), (s, dp_of(yb, z, c))
    to_za, to_zb = (s, dp_of(y, za, c)), (s, dp_of(y, zb, c))
    at_s = {r: (ring(s, r, NS), d) for r in range(1, NS)}

    barrier = pltpu.get_barrier_semaphore()
    greet = [at_s[r] for r in range(1, NS)] + [at_y[r] for r in (1, 2, 3)]
    greet += [at_z[r] for r in (1, 2, 3)] + [at_c]
    for who in greet:
        pl.semaphore_signal(barrier, inc=1, device_id=who, device_id_type=MESH)

    pending = []

    def remote(src, dst, send_sem, recv_sem, who):
        copy = pltpu.make_async_remote_copy(
            src_ref=src, dst_ref=dst, send_sem=send_sem, recv_sem=recv_sem,
            device_id=who, device_id_type=MESH,
        )
        copy.start()
        pending.append(copy)
        return copy

    load_act = pltpu.make_async_copy(act_hbm, act_v, loc.at[0])
    load_acc = pltpu.make_async_copy(acc_hbm, acc_v, loc.at[1])
    own_rows = pl.ds(pl.multiple_of(c * H, 128), H)
    own_lanes = pl.ds(pl.multiple_of(c * HD, 128), HD)
    kv_lanes = pl.ds(pl.multiple_of(2 * HD + c * HD, 128), HD)
    other_rows = pl.ds(pl.multiple_of(o * H, 128), H)
    load_wq = pltpu.make_async_copy(wq_hbm.at[own_rows, :], wbuf.at[:, own_lanes], loc.at[2])
    load_wkv = pltpu.make_async_copy(wkv_hbm.at[own_rows, :], wbuf.at[:, kv_lanes], loc.at[3])
    load_wo = pltpu.make_async_copy(wo_hbm.at[:, own_rows], wobuf.at[c], loc.at[4])
    load_act.start()
    load_acc.start()
    load_wq.start()
    load_wkv.start()
    load_wo.start()

    load_act.wait()
    for r in range(NS):
        to = ring(s, r, NS)
        at = jnp.int32(0)
        for j in range(MB):
            source = sec[to * MB + j]
            at = at + jnp.where((source >> 3) == s, source & 7, 0)
        if r == 0:
            recv_a[s] = act_v[at]
        else:
            asend[r] = act_v[at]
    lsend[...] = jnp.broadcast_to(loss_ref[...], (1, HD))

    pl.semaphore_wait(barrier, len(greet))

    from_s = [
        remote(asend.at[r], recv_a.at[s], a_s.at[r], a_r.at[r], at_s[r]) for r in range(1, NS)
    ]
    from_ly = [
        remote(lsend, lry.at[r], bl_s.at[8 + r], bl_r.at[8 + r], at_y[r]) for r in (1, 2, 3)
    ]
    w_q = remote(wq_hbm.at[other_rows, :], wbuf.at[:, own_lanes], cc_s.at[0], cc_r.at[0], at_c)
    w_kv = remote(wkv_hbm.at[other_rows, :], wbuf.at[:, kv_lanes], cc_s.at[1], cc_r.at[1], at_c)
    w_o = remote(wo_hbm.at[:, other_rows], wobuf.at[c], cc_s.at[2], cc_r.at[2], at_c)

    load_acc.wait()
    from_by = []
    for r in (1, 2, 3, 0):
        base = ring(y, r, NY) * 8

        def pick(k, carry, r=r, base=base):
            first = (base + k) * BLK
            at = jnp.int32(0)
            for b in range(BLK):
                source = blk[first + b]
                at = at + jnp.where((source >> 5) == d, source & 31, 0)
            into = b1.at[0] if r == 0 else bsend.at[r]
            into[lax.div(k, 2), lax.rem(k, 2)] = acc_v[at].astype(BF16)
            return carry

        lax.fori_loop(0, 8, pick, 0)
        if r:
            from_by.append(
                remote(bsend.at[r], b1.at[r], bl_s.at[r], bl_r.at[r], at_y[r])
            )

    for copy in from_s:
        copy.wait_recv()
    x = recv_a[sec[s * MB] >> 3]
    xf = x.astype(F32)
    meansq = jnp.mean(xf * xf, axis=-1, keepdims=True)
    normed = (xf * lax.rsqrt(meansq + EPS) * gpre[...]).astype(BF16)
    nbuf[0] = normed[:, :H]
    nbuf[1] = normed[:, H:]
    xh[y, z, c] = nbuf[c]
    core_n = remote(nbuf.at[o], xh.at[y, z, c], cc_s.at[3], cc_r.at[3], at_c)

    def gather_y(q, zz, h, i):
        piece = xh.at[y, zz, h]
        one = remote(piece, piece, cy_s.at[q, i, 0], cy_r.at[q, i, 0], to_ya)
        two = remote(piece, piece, cy_s.at[q, i, 1], cy_r.at[q, i, 1], to_yb)
        return [one, two]

    def gather_z(h, i):
        piece = xh.at[y, z, h]
        one = remote(piece, piece, cz_s.at[i, 0], cz_r.at[i, 0], to_za)
        two = remote(piece, piece, cz_s.at[i, 1], cz_r.at[i, 1], to_zb)
        return [one, two]

    def pass_y(q, zz, h, i):
        near[q, i][i].wait_recv()
        piece = xh.at[yb if i == 0 else ya, zz, h]
        far[q, i] = remote(
            piece, piece, cy_s.at[q, i, 2], cy_r.at[q, i, 2], to_ya if i == 0 else to_yb
        )

    def pass_z(i):
        zz, h = (zb, c) if i == 0 else (za, o)
        near_z[i][i].wait_recv()
        piece = xh.at[y, zz, h]
        far_z[i] = remote(
            piece, piece, cz_s.at[i, 2], cz_r.at[i, 2], to_za if i == 0 else to_zb
        )

    near, far, near_z, far_z = {}, {}, {}, {}
    order = [z, zb, za, zf]
    near_z[0] = gather_z(c, 0)
    near[0, 0] = gather_y(0, z, c, 0)
    core_n.wait_recv()
    near_z[1] = gather_z(o, 1)
    near[0, 1] = gather_y(0, z, o, 1)
    pass_y(0, z, c, 0)
    pass_z(0)
    near[1, 0] = gather_y(1, zb, c, 0)
    pass_y(0, z, o, 1)
    near_z[0][1].wait_recv()
    near[2, 0] = gather_y(2, za, c, 0)
    pass_z(1)
    near[2, 1] = gather_y(2, za, o, 1)
    near_z[1][0].wait_recv()
    near[1, 1] = gather_y(1, zb, o, 1)
    pass_y(1, zb, c, 0)
    pass_y(2, za, c, 0)

    def project(q):
        zz = order[q]
        near[q, 0][1].wait_recv()
        near[q, 1][0].wait_recv()
        far[q, 0].wait_recv()
        far[q, 1].wait_recv()
        rows = xh[:, zz].reshape(128, H)
        res = jnp.dot(rows, wbuf[...], preferred_element_type=F32)
        for j in range(4):
            rbuf[q, j] = res[:, j * HD : (j + 1) * HD]
        return [
            remote(rbuf.at[q, o], rrq.at[zz], cc_s.at[4 + zz], cc_r.at[4 + zz], at_c),
            remote(rbuf.at[q, pl.ds(2, 2)], rrkv.at[zz], cc_s.at[8 + zz], cc_r.at[8 + zz], at_c),
        ]

    def finish(q, copies):
        zz = order[q]
        for copy in copies:
            copy.wait_recv()
        cosine = tab[0, :, zz].reshape(128, HD)
        sine = tab[1, :, zz].reshape(128, HD)
        query = rbuf[q, c] + rrq[zz]
        key = rbuf[q, 2] + rrkv[zz, 0]
        value = rbuf[q, 3] + rrkv[zz, 1]
        query = query * cosine + pltpu.roll(query, HD // 2, 1) * sine
        key = key * cosine + pltpu.roll(key, HD // 2, 1) * sine
        qf[:, zz] = query.astype(BF16).reshape(NY, 32, HD)
        kf[:, zz] = key.astype(BF16).reshape(NY, 32, HD)
        vf[:, zz] = value.astype(BF16).reshape(NY, 32, HD)

    load_wq.wait()
    load_wkv.wait()
    w_q.wait_recv()
    w_kv.wait_recv()
    shared = {}
    shared[0] = project(0)
    pass_y(2, za, o, 1)
    pass_y(1, zb, o, 1)
    far_z[0].wait_recv()
    near[3, 0] = gather_y(3, zf, c, 0)
    far_z[1].wait_recv()
    near[3, 1] = gather_y(3, zf, o, 1)
    for copy in from_ly:
        copy.wait_recv()
    lsum[...] = lsend[...] + lry[1] + lry[2] + lry[3]
    from_lz = [
        remote(lsum, lrz.at[r], bl_s.at[11 + r], bl_r.at[11 + r], at_z[r]) for r in (1, 2, 3)
    ]
    for copy in from_by:
        copy.wait_recv()
    low, high = pl.ds(0, 2), pl.ds(2, 2)
    b_far = b1.at[:, ring(z, 2, NZ)]
    relay = [
        remote(b_far.at[low], bre.at[0], bz_s.at[0], bz_r.at[0], at_z[1]),
        remote(b_far.at[high], bre.at[1], bz_s.at[1], bz_r.at[1], at_z[-1]),
    ]
    from_bz = [
        remote(b1.at[:, ring(z, 1, NZ)], b2.at[1], bl_s.at[4], bl_r.at[4], at_z[1]),
        remote(b1.at[:, ring(z, 3, NZ)], b2.at[3], bl_s.at[6], bl_r.at[6], at_z[3]),
    ]
    b2[0] = b1[:, z]
    for j in range(MB):
        moved_v[j] = recv_a[sec[s * MB + j] >> 3]
    store_moved = pltpu.make_async_copy(moved_v, moved_hbm, loc.at[5])
    store_moved.start()
    shared[1] = project(1)
    finish(0, shared[0])
    pass_y(3, zf, c, 0)
    shared[2] = project(2)
    pass_y(3, zf, o, 1)
    finish(1, shared[1])
    finish(2, shared[2])
    relay[0].wait_recv()
    from_bz.append(
        remote(bre.at[0], b2.at[2, low], bz_s.at[2], bz_r.at[2], at_z[1])
    )
    relay[1].wait_recv()
    from_bz.append(
        remote(bre.at[1], b2.at[2, high], bz_s.at[3], bz_r.at[3], at_z[-1])
    )
    shared[3] = project(3)
    finish(3, shared[3])
    back = [zf, zb, za, z]
    keys, values = kf[...].reshape(512, HD), vf[...].reshape(512, HD)
    line = lax.broadcasted_iota(jnp.int32, (128, 512), 0)
    token = ((line >> 5) << 7) + (line & 31)
    col = lax.broadcasted_iota(jnp.int32, (128, 512), 1)
    from_att = []
    for m in range(4):
        scores = lax.dot_general(
            qf[:, back[m]].reshape(128, HD), keys,
            (((1,), (1,)), ((), ())), preferred_element_type=F32,
        ) * ((D / 32) ** (-0.5))
        capped = 50.0 * jnp.tanh(scores / 50.0)
        expd = jnp.where(col <= token + back[m] * 32, jnp.exp(capped), 0.0)
        total = jnp.sum(expd, axis=-1, keepdims=True)
        numer = jnp.dot(expd.astype(BF16), values, preferred_element_type=F32)
        zz = back[m]
        at2[c, zz] = (numer / total).astype(BF16)
        from_att.append(
            remote(at2.at[c, zz], at2.at[c, zz], cc_s.at[12 + zz], cc_r.at[12 + zz], at_c)
        )

    load_wo.wait()
    w_o.wait_recv()
    y_far, y_own, y_mid = {}, {}, {}

    def part(q):
        from_att[q].wait_recv()
        res = jnp.dot(at2[0, back[q]], wobuf[0], preferred_element_type=F32)
        res = res + jnp.dot(at2[1, back[q]], wobuf[1], preferred_element_type=F32)
        pbuf[:, back[q]] = res.astype(BF16).reshape(NY, 2, ROWS, H)

    def issue(q, i):
        zz, h = back[q], (c, o)[i]
        first, second = ((to_ya, to_yb), (to_yb, to_ya))[i]
        y_far[q, i] = remote(
            pbuf.at[yf, zz, h], yrh.at[q, i], dy_s.at[q, i, 0], dy_r.at[q, i, 0], first
        )
        y_own[q, i] = remote(
            pbuf.at[(yb, ya)[i], zz, h], yro.at[q, i], dy_s.at[q, i, 1], dy_r.at[q, i, 1], second
        )

    def middle(q, i):
        zz, h = back[q], (c, o)[i]
        next_y, who = ((ya, to_ya), (yb, to_yb))[i]
        y_far[q, i].wait_recv()
        total = pbuf[next_y, zz, h].astype(F32) + yrh[q, i].astype(F32)
        pbuf[next_y, zz, h] = total.astype(BF16)
        y_mid[q, i] = remote(
            pbuf.at[next_y, zz, h], yrm.at[q, i], dy_s.at[q, i, 2], dy_r.at[q, i, 2], who
        )

    def reduced(q, i):
        y_own[q, i].wait_recv()
        y_mid[q, i].wait_recv()
        total = pbuf[y, back[q], (c, o)[i]].astype(F32)
        return total + yro[q, i].astype(F32) + yrm[q, i].astype(F32)

    def send_z(value, kind, i, into, who):
        zs[kind, i] = value.astype(BF16)
        return remote(
            zs.at[kind, i], into.at[i], dz_s.at[kind, i], dz_r.at[kind, i], who
        )

    part(0)
    issue(0, 0)
    issue(0, 1)
    part(1)
    issue(1, 0)
    part(2)
    issue(2, 1)
    middle(0, 0)
    middle(0, 1)
    issue(2, 0)
    issue(1, 1)
    middle(1, 0)
    middle(2, 1)
    part(3)
    z_far = [send_z(reduced(0, 0), 0, 0, zrh, to_za)]
    z_far.append(send_z(reduced(0, 1), 0, 1, zrh, to_zb))
    issue(3, 0)
    issue(3, 1)
    middle(2, 0)
    middle(1, 1)
    z_own = [send_z(reduced(1, 0), 1, 0, zro, to_zb)]
    z_own.append(send_z(reduced(2, 1), 1, 1, zro, to_za))
    middle(3, 0)
    middle(3, 1)
    total = reduced(2, 0)
    z_far[0].wait_recv()
    z_mid = [send_z(total + zrh[0].astype(F32), 2, 0, zrm, to_za)]
    total = reduced(1, 1)
    z_far[1].wait_recv()
    z_mid.append(send_z(total + zrh[1].astype(F32), 2, 1, zrm, to_zb))

    for copy in from_bz + from_lz:
        copy.wait_recv()
    core_b = remote(b2.at[:, :, o], b3, bl_s.at[7], bl_r.at[7], at_c)
    lfin[...] = lsum[...] + lrz[1] + lrz[2] + lrz[3]
    core_l = remote(lfin, lrc, bl_s.at[15], bl_r.at[15], at_c)

    core_l.wait_recv()
    core_b.wait_recv()
    factor = 32.0 / (lfin[...] + lrc[...])[0, 0]

    def place(b, carry):
        source = blk[d * BLK + b] >> 5
        ry = (y - (source >> 3)) & 3
        rz = (z - ((source >> 1) & 3)) & 3
        mine = b2[rz, ry, c].astype(F32)
        theirs = b3[rz, ry].astype(F32)
        newacc_v[b] = jnp.where((source & 1) == c, mine, theirs) * factor
        return carry

    lax.fori_loop(0, BLK, place, 0)
    store_acc = pltpu.make_async_copy(newacc_v, newacc_hbm, loc.at[6])
    store_acc.start()

    sums = [reduced(3, 0), reduced(3, 1)]
    for i in range(2):
        z_own[i].wait_recv()
        z_mid[i].wait_recv()
        fb[i] = sums[i] + zro[i].astype(F32) + zrm[i].astype(F32)
    last = remote(fb.at[1], finr, cc_s.at[16], cc_r.at[16], at_c)
    checked = recv_a[sec[s * MB] >> 3].astype(F32)
    last.wait_recv()
    mine = fb[0]
    theirs = finr[...]
    meansq = jnp.sum(mine * mine, axis=-1, keepdims=True)
    meansq = (meansq + jnp.sum(theirs * theirs, axis=-1, keepdims=True)) / D
    scale = lax.rsqrt(meansq + EPS)
    outb[c] = mine
    outb[o] = theirs
    for h in range(2):
        cols = slice(h * H, (h + 1) * H)
        checkb[h] = (checked[:, cols] + outb[h] * scale * gpost[:, cols]).astype(BF16)
    stores = [
        pltpu.make_async_copy(checkb.at[h], check_hbm.at[:, pl.ds(h * H, H)], loc.at[7 + h])
        for h in range(2)
    ]
    for copy in stores:
        copy.start()
    for copy in pending:
        copy.wait_send()
    for copy in [store_moved, store_acc] + stores:
        copy.wait()


def on_device(act, sec, acc, blk, loss, gpre, wq, wkv, wo, gpost):
    tab = jnp.asarray(rotary_tables())
    any_ = pl.BlockSpec(memory_space=pl.ANY)
    smem = pl.BlockSpec(memory_space=pltpu.SMEM)
    vmem = pl.BlockSpec(memory_space=pltpu.VMEM)
    V = pltpu.VMEM
    dma = pltpu.SemaphoreType.DMA
    moved, newacc, check = pl.pallas_call(
        kernel,
        out_shape=(
            jax.ShapeDtypeStruct((MB, ROWS, D), BF16),
            jax.ShapeDtypeStruct((BLK, 2, D), F32),
            jax.ShapeDtypeStruct((ROWS, D), BF16),
        ),
        in_specs=[smem, smem, any_, any_, vmem, vmem, any_, any_, any_, vmem, vmem],
        out_specs=(any_, any_, any_),
        scratch_shapes=[
            V((MB, ROWS, D), BF16), V((NS, ROWS, D), BF16), V((NS, ROWS, D), BF16),
            V((MB, ROWS, D), BF16), V((BLK, 2, D), F32),
            V((NY, NZ, 2, 2, D), BF16), V((NY, NZ, 2, 2, D), BF16),
            V((NZ, NY, 2, 2, D), BF16), V((NZ, NY, 2, D), BF16), V((2, 2, 2, 2, D), BF16), V((BLK, 2, D), F32),
            V((1, HD), F32), V((4, 1, HD), F32), V((1, HD), F32), V((4, 1, HD), F32),
            V((1, HD), F32), V((1, HD), F32),
            V((2, ROWS, H), BF16), V((NY, NZ, 2, ROWS, H), BF16), V((H, 4 * HD), BF16),
            V((2, HD, H), BF16), V((4, 4, 128, HD), F32), V((4, 128, HD), F32),
            V((4, 2, 128, HD), F32), V((NY, NZ, 32, HD), BF16), V((NY, NZ, 32, HD), BF16),
            V((NY, NZ, 32, HD), BF16), V((2, 4, 128, HD), BF16),
            V((NY, NZ, 2, ROWS, H), BF16), V((4, 2, ROWS, H), BF16), V((4, 2, ROWS, H), BF16),
            V((4, 2, ROWS, H), BF16), V((2, ROWS, H), BF16), V((2, ROWS, H), BF16),
            V((2, ROWS, H), BF16), V((3, 2, ROWS, H), BF16), V((2, ROWS, H), F32),
            V((ROWS, H), F32), V((2, ROWS, H), F32), V((2, ROWS, H), BF16),
            dma((9,)), dma((NS,)), dma((NS,)), dma((16,)), dma((16,)), dma((2, 3)), dma((2, 3)),
            dma((4, 2, 3)), dma((4, 2, 3)), dma((17,)), dma((17,)),
            dma((4, 2, 3)), dma((4, 2, 3)), dma((3, 2)), dma((3, 2)), dma((4,)), dma((4,)),
        ],
        compiler_params=pltpu.CompilerParams(
            collective_id=0, has_side_effects=True, vmem_limit_bytes=60 * 1024 * 1024
        ),
        name="restore",
    )(sec, blk, act, acc, loss, gpre, wq[0], wkv[0], wo[0], gpost, tab)
    return moved, newacc, check[None]


def solution(mesh):
    placed = (
        P("section", "dp", None),
        P(),
        P("dp", "section", None),
        P(),
        P("section", "dp"),
        P("section", None),
        P("section", None, "dp"),
        P("section", None, "dp"),
        P("section", "dp", None),
        P("section", None),
    )
    return jax.shard_map(
        on_device,
        mesh=mesh,
        in_specs=placed,
        out_specs=(P("section", "dp", None), P("dp", "section", None), P("section", "dp", None)),
        check_vma=False,
    )
```

```python
import functools

import jax
import jax.numpy as jnp
import numpy as np
from jax import lax
from jax.experimental import pallas as pl
from jax.experimental.pallas import tpu as pltpu
from jax.sharding import PartitionSpec as P

MESH = pl.DeviceIdType.MESH
D = 4608
H = D // 2
HD = 128
NS = 8
NY = 4
NZ = 4
MB = 8
ROWS = 16
BLK = 32
EPS = 1e-06
NP = 2
HP = H // NP
F32 = jnp.float32
BF16 = jnp.bfloat16

GATHER = (
    ("near", 0, 1), ("row", 0, 0, 1), ("row", 0, 0, 0), ("near", 0, 0), ("near", 1, 1),
    ("row", 0, 1, 0), ("row", 0, 1, 1), ("near", 1, 0), ("ony", 0, 0, 1), ("ony", 0, 0, 0),
    ("row", 1, 0, 1), ("ony", 0, 1, 0), ("ony", 0, 1, 1), ("row", 2, 0, 1), ("row", 1, 0, 0),
    ("row", 2, 0, 0), ("onz", 0, 0), ("onz", 0, 1), ("row", 2, 1, 1), ("row", 1, 1, 1),
    ("moved",), ("onz", 1, 1), ("onz", 1, 0), ("ony", 2, 0, 1), ("project", 0), ("row", 1, 1, 0),
    ("ony", 1, 0, 1), ("row", 2, 1, 0), ("blocks",), ("row", 3, 1, 1), ("ony", 1, 0, 0),
    ("ony", 1, 1, 1), ("ony", 1, 1, 0), ("ony", 2, 1, 1), ("row", 3, 1, 0), ("ony", 2, 1, 0),
    ("row", 3, 0, 0), ("row", 3, 0, 1), ("ony", 2, 0, 0), ("ony", 3, 1, 1), ("ony", 3, 1, 0),
    ("relay",), ("ony", 3, 0, 0), ("ony", 3, 0, 1), ("project", 1), ("finish", 0), ("project", 2),
    ("project", 3), ("finish", 1), ("finish", 2), ("finish", 3),
)

REDUCE = (
    ("part", 0), ("far", 0, 0, 0), ("far", 0, 0, 1), ("part", 1), ("far", 1, 0, 0),
    ("side", 1, 1, 0), ("side", 1, 0, 0), ("attend", 3), ("own", 0, 0, 0), ("side", 1, 0, 1),
    ("side", 1, 1, 1), ("far", 0, 1, 0), ("far", 1, 1, 0), ("far", 0, 1, 1), ("middle", 0, 0, 0),
    ("far", 1, 0, 1), ("part", 2), ("own", 0, 1, 1), ("far", 2, 0, 0), ("own", 0, 1, 0),
    ("side", 2, 1, 0), ("side", 2, 1, 1), ("middle", 0, 1, 0), ("own", 0, 0, 1), ("part", 3),
    ("middle", 0, 0, 1), ("side", 2, 0, 1), ("zfar", 0, 0), ("cores",), ("middle", 0, 1, 1),
    ("side", 2, 0, 0), ("far", 2, 1, 1), ("middle", 2, 0, 0), ("middle", 1, 0, 0), ("zfar", 1, 0),
    ("far", 1, 1, 1), ("middle", 1, 0, 1), ("zfar", 0, 1), ("far", 2, 1, 0), ("middle", 1, 1, 0),
    ("zfar", 1, 1), ("middle", 2, 1, 1), ("far", 2, 0, 1), ("far", 3, 1, 1), ("far", 3, 0, 0),
    ("zmid", 0, 0), ("zown", 0, 0), ("middle", 1, 1, 1), ("middle", 2, 1, 0), ("far", 3, 1, 0),
    ("own", 3, 0, 0), ("zown", 0, 1), ("zmid", 1, 0), ("middle", 2, 0, 1), ("far", 3, 0, 1),
    ("zown", 1, 1), ("middle", 3, 0, 0), ("own", 3, 1, 1), ("own", 3, 1, 0), ("zmid", 1, 1),
    ("place",), ("middle", 3, 1, 0), ("middle", 3, 1, 1), ("zown", 1, 0), ("own", 3, 0, 1),
    ("zmid", 0, 1), ("middle", 3, 0, 1), ("finish", 1, 1), ("finish", 0, 0), ("finish", 1, 0),
    ("finish", 0, 1),
)


def rotary_tables():
    freqs = (10000.0 ** (-2.0 * np.arange(HD // 2, dtype=np.float32) / HD)).astype(np.float32)
    angles = np.arange(512, dtype=np.float32)[:, None] * freqs[None, :]
    cosine, sine = np.cos(angles), np.sin(angles)
    full = np.stack(
        [np.concatenate([cosine, cosine], axis=1), np.concatenate([-sine, sine], axis=1)]
    )
    return full.astype(np.float32).reshape(2, NY, NZ, 32, HD)


def kernel(
    sec_hbm, blk_hbm, act_hbm, acc_hbm, loss_hbm, gpre_hbm, wq_hbm, wkv_hbm, wo_hbm, gpost_hbm, tab_hbm,
    moved_v, newacc_v, checkb,
    act_v, asend, recv_a, acc_v, bsend, b1, b2, b3, bre,
    lsend, lry, lsum, lrz, lfin, lrc,
    nbuf, xh, wbuf, wobuf, rbuf, rrq, rrkv, qf, kf, vf, at2,
    pbuf, yrh, yro, yrm, zrh, zro, zrm, zs, fb, finr, outb, tab, sec, blk, loss_ref, gpre, gpost,
    zrs, loc, df_s, df_r, dx_s, dx_r, a_s, a_r, bl_s, bl_r, cz_s, cz_r, cy_s, cy_r, cc_s, cc_r, dy_s, dy_r, dz_s, dz_r, bz_s, bz_r,
):
    s = lax.axis_index("section")
    d = lax.axis_index("dp")
    y = lax.div(d, 8)
    z = lax.rem(lax.div(d, 2), 4)
    c = lax.rem(d, 2)
    o = 1 - c

    def ring(v, r, n):
        return lax.rem(v + (r + n), n)

    def dp_of(yy, zz, cc):
        return (yy * NZ + zz) * 2 + cc

    at_y = {r: (s, dp_of(ring(y, r, NY), z, c)) for r in (1, 2, 3, -1)}
    at_z = {r: (s, dp_of(y, ring(z, r, NZ), c)) for r in (1, 2, 3, -1)}
    at_c = (s, dp_of(y, z, o))
    ahead = 1 - 2 * c
    ya, yb, yf = ring(y, ahead, NY), ring(y, -ahead, NY), ring(y, 2, NY)
    za, zb, zf = ring(z, ahead, NZ), ring(z, -ahead, NZ), ring(z, 2, NZ)
    to_ya, to_yb = (s, dp_of(ya, z, c)), (s, dp_of(yb, z, c))
    to_za, to_zb = (s, dp_of(y, za, c)), (s, dp_of(y, zb, c))
    at_s = {r: (ring(s, r, NS), d) for r in range(1, NS)}

    barrier = pltpu.get_barrier_semaphore()
    greet = [at_s[r] for r in range(1, NS)] + [at_y[r] for r in (1, 2, 3)]
    greet += [at_z[r] for r in (1, 2, 3)] + [at_c]
    for who in greet:
        pl.semaphore_signal(barrier, inc=1, device_id=who, device_id_type=MESH)

    pending, seen = [], set()

    def arrived(copy):
        if id(copy) not in seen:
            seen.add(id(copy))
            copy.wait_recv()

    def remote(src, dst, send_sem, recv_sem, who):
        copy = pltpu.make_async_remote_copy(
            src_ref=src, dst_ref=dst, send_sem=send_sem, recv_sem=recv_sem,
            device_id=who, device_id_type=MESH,
        )
        copy.start()
        pending.append(copy)
        return copy

    load_act = pltpu.make_async_copy(act_hbm, act_v, loc.at[0])
    load_acc = pltpu.make_async_copy(acc_hbm, acc_v, loc.at[1])
    own_rows = pl.ds(pl.multiple_of(c * H, 128), H)
    own_lanes = pl.ds(pl.multiple_of(c * HD, 128), HD)
    kv_lanes = pl.ds(pl.multiple_of(2 * HD + c * HD, 128), HD)
    other_rows = pl.ds(pl.multiple_of(o * H, 128), H)
    load_wq = pltpu.make_async_copy(wq_hbm.at[own_rows, :], wbuf.at[:, own_lanes], loc.at[2])
    load_wkv = pltpu.make_async_copy(wkv_hbm.at[own_rows, :], wbuf.at[:, kv_lanes], loc.at[3])
    load_wo = pltpu.make_async_copy(wo_hbm.at[:, own_rows], wobuf.at[c], loc.at[4])
    load_tab = pltpu.make_async_copy(tab_hbm, tab, loc.at[9])
    small = [
        pltpu.make_async_copy(source, into, loc.at[10 + i])
        for i, (source, into) in enumerate(
            ((sec_hbm, sec), (loss_hbm, loss_ref), (blk_hbm, blk), (gpre_hbm, gpre),
             (gpost_hbm, gpost))
        )
    ]
    load_act.start()
    for copy in small:
        copy.start()
    load_acc.start()
    load_wq.start()
    load_wkv.start()
    load_wo.start()
    load_tab.start()

    load_act.wait()
    small[0].wait()
    small[1].wait()
    for r in range(NS):
        to = ring(s, r, NS)
        at = jnp.int32(0)
        for j in range(MB):
            source = sec[to * MB + j]
            at = at + jnp.where((source >> 3) == s, source & 7, 0)
        if r == 0:
            recv_a[s] = act_v[at]
        else:
            asend[r] = act_v[at]
    lsend[...] = jnp.broadcast_to(loss_ref[...], (1, HD))

    pl.semaphore_wait(barrier, len(greet))

    from_s = [
        remote(asend.at[r], recv_a.at[s], a_s.at[r], a_r.at[r], at_s[r]) for r in range(1, NS)
    ]
    from_ly = [
        remote(lsend, lry.at[r], bl_s.at[8 + r], bl_r.at[8 + r], at_y[r]) for r in (1, 2, 3)
    ]
    w_q = remote(wq_hbm.at[other_rows, :], wbuf.at[:, own_lanes], cc_s.at[0], cc_r.at[0], at_c)
    w_kv = remote(wkv_hbm.at[other_rows, :], wbuf.at[:, kv_lanes], cc_s.at[1], cc_r.at[1], at_c)
    w_o = remote(wo_hbm.at[:, other_rows], wobuf.at[c], cc_s.at[2], cc_r.at[2], at_c)

    load_acc.wait()
    for copy in small[2:]:
        copy.wait()
    from_by = []
    for r in (1, 2, 3, 0):
        base = ring(y, r, NY) * 8

        def pick(k, carry, r=r, base=base):
            first = (base + k) * BLK
            at = jnp.int32(0)
            for b in range(BLK):
                source = blk[first + b]
                at = at + jnp.where((source >> 5) == d, source & 31, 0)
            into = b1.at[0] if r == 0 else bsend.at[r]
            into[lax.div(k, 2), lax.rem(k, 2)] = acc_v[at].astype(BF16)
            return carry

        lax.fori_loop(0, 8, pick, 0)
        if r:
            from_by.append(
                remote(bsend.at[r], b1.at[r], bl_s.at[r], bl_r.at[r], at_y[r])
            )

    for copy in from_s:
        copy.wait_recv()
    x = recv_a[sec[s * MB] >> 3]
    xf = x.astype(F32)
    meansq = jnp.mean(xf * xf, axis=-1, keepdims=True)
    normed = (xf * lax.rsqrt(meansq + EPS) * gpre[...]).astype(BF16)
    nbuf[0] = normed[:, :H]
    nbuf[1] = normed[:, H:]
    xh[y, z, c] = nbuf[c]
    core_n = remote(nbuf.at[o], xh.at[y, z, c], cc_s.at[3], cc_r.at[3], at_c)

    half = (c, o)

    def piece_of(yy, zz, i, p):
        return xh.at[yy, zz, half[i], :, pl.ds(p * HP, HP)]

    order = [z, zb, za, zf]
    near_z, far_z, rows_y, rows_on = {}, {}, {}, {}

    def do_near(i, p):
        piece = piece_of(y, z, i, p)
        for way, who in enumerate((to_za, to_zb)):
            near_z[i, p, way] = remote(
                piece, piece, cz_s.at[i, way, p], cz_r.at[i, way, p], who
            )

    def do_row(q, i, p):
        if q == 1 or q == 2:
            arrived(near_z[i, p, q - 1])
        if q == 3:
            far_z[i, p].wait_recv()
        piece = piece_of(y, order[q], i, p)
        for way, who in enumerate((to_ya, to_yb)):
            rows_y[q, i, p, way] = remote(
                piece, piece, cy_s.at[q, i, way, p], cy_r.at[q, i, way, p], who
            )

    def do_onz(i, p):
        arrived(near_z[i, p, i])
        piece = piece_of(y, (zb, za)[i], i, p)
        far_z[i, p] = remote(
            piece, piece, cz_s.at[i, 2, p], cz_r.at[i, 2, p], (to_za, to_zb)[i]
        )

    def do_ony(q, i, p):
        rows_y[q, i, p, i].wait_recv()
        piece = piece_of((yb, ya)[i], order[q], i, p)
        rows_on[q, i, p] = remote(
            piece, piece, cy_s.at[q, i, 2, p], cy_r.at[q, i, 2, p], (to_ya, to_yb)[i]
        )

    def do_project(q):
        if q == 0:
            load_tab.wait()
            load_wq.wait()
            load_wkv.wait()
            w_q.wait_recv()
            w_kv.wait_recv()
        zz = order[q]
        for i in range(2):
            for p in range(NP):
                rows_y[q, i, p, 1 - i].wait_recv()
                rows_on[q, i, p].wait_recv()
        rows = xh[:, zz].reshape(128, H)
        res = jnp.dot(rows, wbuf[...], preferred_element_type=F32)
        for j in range(4):
            rbuf[q, j] = res[:, j * HD : (j + 1) * HD]
        shared[q] = [
            remote(rbuf.at[q, o], rrq.at[zz], cc_s.at[4 + zz], cc_r.at[4 + zz], at_c),
            remote(rbuf.at[q, pl.ds(2, 2)], rrkv.at[zz], cc_s.at[8 + zz], cc_r.at[8 + zz], at_c),
        ]

    def do_finish(q):
        zz = order[q]
        for copy in shared[q]:
            copy.wait_recv()
        cosine = tab[0, :, zz].reshape(128, HD)
        sine = tab[1, :, zz].reshape(128, HD)
        query = rbuf[q, c] + rrq[zz]
        key = rbuf[q, 2] + rrkv[zz, 0]
        value = rbuf[q, 3] + rrkv[zz, 1]
        query = query * cosine + pltpu.roll(query, HD // 2, 1) * sine
        key = key * cosine + pltpu.roll(key, HD // 2, 1) * sine
        qf[:, zz] = query.astype(BF16).reshape(NY, 32, HD)
        kf[:, zz] = key.astype(BF16).reshape(NY, 32, HD)
        vf[:, zz] = value.astype(BF16).reshape(NY, 32, HD)

    shared, relay, from_lz, from_bz = {}, [], [], []
    low, high = pl.ds(0, 2), pl.ds(2, 2)

    def do_blocks():
        for copy in from_ly:
            copy.wait_recv()
        lsum[...] = lsend[...] + lry[1] + lry[2] + lry[3]
        from_lz.extend(
            remote(lsum, lrz.at[r], bl_s.at[11 + r], bl_r.at[11 + r], at_z[r])
            for r in (1, 2, 3)
        )
        for copy in from_by:
            copy.wait_recv()
        b_far = b1.at[:, ring(z, 2, NZ)]
        relay.append(remote(b_far.at[low], bre.at[0], bz_s.at[0], bz_r.at[0], at_z[1]))
        relay.append(remote(b_far.at[high], bre.at[1], bz_s.at[1], bz_r.at[1], at_z[-1]))
        for r in (1, 3):
            from_bz.append(
                remote(b1.at[:, ring(z, r, NZ)], b2.at[r], bl_s.at[3 + r], bl_r.at[3 + r], at_z[r])
            )
        b2[0] = b1[:, z]

    def do_relay():
        for i, (part_of, who) in enumerate(((low, at_z[1]), (high, at_z[-1]))):
            relay[i].wait_recv()
            from_bz.append(
                remote(bre.at[i], b2.at[2, part_of], bz_s.at[2 + i], bz_r.at[2 + i], who)
            )

    def do_moved():
        for j in range(MB):
            moved_v[j] = recv_a[sec[s * MB + j] >> 3]

    steps = dict(
        near=do_near, row=do_row, onz=do_onz, ony=do_ony, project=do_project,
        finish=do_finish, blocks=do_blocks, relay=do_relay, moved=do_moved,
    )
    waited = False
    for name, *which in GATHER:
        second = (name == "near" and which[0] == 1) or (name == "row" and which[:2] == [0, 1])
        if second and not waited:
            core_n.wait_recv()
            waited = True
        with jax.named_scope("_".join([name] + [str(w) for w in which])):
            steps[name](*which)
    back = [zf, zb, za, z]
    keys, values = kf[...].reshape(512, HD), vf[...].reshape(512, HD)
    line = lax.broadcasted_iota(jnp.int32, (128, 512), 0)
    token = ((line >> 5) << 7) + (line & 31)
    col = lax.broadcasted_iota(jnp.int32, (128, 512), 1)
    from_att = {}

    def do_attend(m):
        scores = lax.dot_general(
            qf[:, back[m]].reshape(128, HD), keys,
            (((1,), (1,)), ((), ())), preferred_element_type=F32,
        ) * ((D / 32) ** (-0.5))
        capped = 50.0 * jnp.tanh(scores / 50.0)
        expd = jnp.where(col <= token + back[m] * 32, jnp.exp(capped), 0.0)
        total = jnp.sum(expd, axis=-1, keepdims=True)
        numer = jnp.dot(expd.astype(BF16), values, preferred_element_type=F32)
        zz = back[m]
        at2[c, zz] = (numer / total).astype(BF16)
        from_att[m] = remote(
            at2.at[c, zz], at2.at[c, zz], cc_s.at[12 + zz], cc_r.at[12 + zz], at_c
        )

    for m in range(3):
        do_attend(m)

    y_far, y_own, y_mid, z_side, z_far, z_own, z_mid, late = {}, {}, {}, {}, {}, {}, {}, {}

    def cols(p):
        return pl.ds(p * HP, HP)

    def mine_at(yy, q, i, p):
        return pbuf.at[yy, back[q], half[i], :, cols(p)]

    def do_part(q):
        if q == 0:
            load_wo.wait()
            w_o.wait_recv()
        from_att[q].wait_recv()
        res = jnp.dot(at2[0, back[q]], wobuf[0], preferred_element_type=F32)
        res = res + jnp.dot(at2[1, back[q]], wobuf[1], preferred_element_type=F32)
        pbuf[:, back[q]] = res.astype(BF16).reshape(NY, 2, ROWS, H)

    def do_far(q, i, p):
        y_far[q, i, p] = remote(
            mine_at(yf, q, i, p), yrh.at[q, i, :, cols(p)],
            dy_s.at[q, i, 0, p], dy_r.at[q, i, 0, p], (to_ya, to_yb)[i],
        )

    def do_own(q, i, p):
        source = mine_at((yb, ya)[i], q, i, p)
        if q == 3:
            z_side[1, i, p].wait_recv()
            z_side[2, i, p].wait_recv()
            total = source[...].astype(F32) + zrs[0, i, :, cols(p)].astype(F32)
            source[...] = (total + zrs[1, i, :, cols(p)].astype(F32)).astype(BF16)
        y_own[q, i, p] = remote(
            source, yro.at[q, i, :, cols(p)],
            dy_s.at[q, i, 1, p], dy_r.at[q, i, 1, p], (to_yb, to_ya)[i],
        )

    def do_side(q, i, p):
        z_side[q, i, p] = remote(
            mine_at((yb, ya)[i], q, i, p), zrs.at[q - 1, i, :, cols(p)],
            dx_s.at[q - 1, i, p], dx_r.at[q - 1, i, p], (to_zb, to_za)[q - 1],
        )

    def do_middle(q, i, p):
        y_far[q, i, p].wait_recv()
        source = mine_at((ya, yb)[i], q, i, p)
        total = source[...].astype(F32) + yrh[q, i, :, cols(p)].astype(F32)
        source[...] = total.astype(BF16)
        y_mid[q, i, p] = remote(
            source, yrm.at[q, i, :, cols(p)],
            dy_s.at[q, i, 2, p], dy_r.at[q, i, 2, p], (to_ya, to_yb)[i],
        )

    def reduced(q, i, p):
        total = mine_at(y, q, i, p)[...].astype(F32)
        if q == 0 or q == 3:
            y_own[q, i, p].wait_recv()
            total = total + yro[q, i, :, cols(p)].astype(F32)
        y_mid[q, i, p].wait_recv()
        return total + yrm[q, i, :, cols(p)].astype(F32)

    def send_z(value, kind, i, p, into, who):
        zs[kind, i, :, cols(p)] = value.astype(BF16)
        return remote(
            zs.at[kind, i, :, cols(p)], into.at[i, :, cols(p)],
            dz_s.at[kind, i, p], dz_r.at[kind, i, p], who,
        )

    def do_zfar(i, p):
        z_far[i, p] = send_z(reduced(0, i, p), 0, i, p, zrh, (to_za, to_zb)[i])

    def do_zown(i, p):
        z_own[i, p] = send_z(reduced(1 + i, i, p), 1, i, p, zro, (to_zb, to_za)[i])

    def do_zmid(i, p):
        total = reduced(2 - i, i, p)
        z_far[i, p].wait_recv()
        total = total + zrh[i, :, cols(p)].astype(F32)
        z_mid[i, p] = send_z(total, 2, i, p, zrm, (to_za, to_zb)[i])

    def do_cores():
        for copy in from_bz + from_lz:
            copy.wait_recv()
        late["blocks"] = remote(b2.at[:, :, o], b3, bl_s.at[7], bl_r.at[7], at_c)
        lfin[...] = lsum[...] + lrz[1] + lrz[2] + lrz[3]
        late["loss"] = remote(lfin, lrc, bl_s.at[15], bl_r.at[15], at_c)

    def do_place():
        late["loss"].wait_recv()
        late["blocks"].wait_recv()
        factor = 32.0 / (lfin[...] + lrc[...])[0, 0]

        def place(b, carry):
            source = blk[d * BLK + b] >> 5
            ry = (y - (source >> 3)) & 3
            rz = (z - ((source >> 1) & 3)) & 3
            mine = b2[rz, ry, c].astype(F32)
            theirs = b3[rz, ry].astype(F32)
            newacc_v[b] = jnp.where((source & 1) == c, mine, theirs) * factor
            return carry

        lax.fori_loop(0, BLK, place, 0)

    def do_finish_sum(i, p):
        total = reduced(3, i, p)
        z_own[i, p].wait_recv()
        z_mid[i, p].wait_recv()
        total = total + zro[i, :, cols(p)].astype(F32)
        fb[i, :, cols(p)] = total + zrm[i, :, cols(p)].astype(F32)
        if i == 1:
            late[p] = remote(
                fb.at[1, :, cols(p)], finr.at[:, cols(p)], df_s.at[p], df_r.at[p], at_c
            )

    steps = dict(
        part=do_part, far=do_far, own=do_own, side=do_side, middle=do_middle, zfar=do_zfar,
        zown=do_zown, zmid=do_zmid, cores=do_cores, place=do_place, finish=do_finish_sum,
        attend=do_attend,
    )
    for name, *which in REDUCE:
        with jax.named_scope("_".join([name] + [str(w) for w in which])):
            steps[name](*which)
    checked = recv_a[sec[s * MB] >> 3].astype(F32)
    for p in range(NP):
        late[p].wait_recv()
    mine = fb[0]
    theirs = finr[...]
    meansq = jnp.sum(mine * mine, axis=-1, keepdims=True)
    meansq = (meansq + jnp.sum(theirs * theirs, axis=-1, keepdims=True)) / D
    scale = lax.rsqrt(meansq + EPS)
    outb[c] = mine
    outb[o] = theirs
    for h in range(2):
        cols_of = slice(h * H, (h + 1) * H)
        checkb[:, cols_of] = (checked[:, cols_of] + outb[h] * scale * gpost[:, cols_of]).astype(BF16)
    for copy in pending:
        copy.wait_send()


def put_out(moved, newacc, check, moved_hbm, newacc_hbm, check_hbm, sem):
    copies = [
        pltpu.make_async_copy(source, into, sem.at[i])
        for i, (source, into) in enumerate(
            ((newacc, newacc_hbm), (moved, moved_hbm), (check, check_hbm))
        )
    ]
    for copy in copies:
        copy.start()
    for copy in copies:
        copy.wait()


def on_device(act, sec, acc, blk, loss, gpre, wq, wkv, wo, gpost):
    tab = jnp.asarray(rotary_tables())
    any_ = pl.BlockSpec(memory_space=pl.ANY)
    vmem = pl.BlockSpec(memory_space=pltpu.VMEM)
    V = pltpu.VMEM
    dma = pltpu.SemaphoreType.DMA
    moved, newacc, check = pl.pallas_call(
        kernel,
        out_shape=(
            V((MB, ROWS, D), BF16),
            V((BLK, 2, D), F32),
            V((ROWS, D), BF16),
        ),
        in_specs=[pl.BlockSpec(memory_space=pltpu.HBM)] * 11,
        out_specs=(vmem, vmem, vmem),
        scratch_shapes=[
            V((MB, ROWS, D), BF16), V((NS, ROWS, D), BF16), V((NS, ROWS, D), BF16),
            V((BLK, 2, D), F32),
            V((NY, NZ, 2, 2, D), BF16), V((NY, NZ, 2, 2, D), BF16),
            V((NZ, NY, 2, 2, D), BF16), V((NZ, NY, 2, D), BF16), V((2, 2, 2, 2, D), BF16),
            V((1, HD), F32), V((4, 1, HD), F32), V((1, HD), F32), V((4, 1, HD), F32),
            V((1, HD), F32), V((1, HD), F32),
            V((2, ROWS, H), BF16), V((NY, NZ, 2, ROWS, H), BF16), V((H, 4 * HD), BF16),
            V((2, HD, H), BF16), V((4, 4, 128, HD), F32), V((4, 128, HD), F32),
            V((4, 2, 128, HD), F32), V((NY, NZ, 32, HD), BF16), V((NY, NZ, 32, HD), BF16),
            V((NY, NZ, 32, HD), BF16), V((2, 4, 128, HD), BF16),
            V((NY, NZ, 2, ROWS, H), BF16), V((4, 2, ROWS, H), BF16), V((4, 2, ROWS, H), BF16),
            V((4, 2, ROWS, H), BF16), V((2, ROWS, H), BF16), V((2, ROWS, H), BF16),
            V((2, ROWS, H), BF16), V((3, 2, ROWS, H), BF16), V((2, ROWS, H), F32),
            V((ROWS, H), F32), V((2, ROWS, H), F32),
            V((2, NY, NZ, 32, HD), F32), pltpu.SMEM((64,), jnp.int32),
            pltpu.SMEM((1024,), jnp.int32), V((1, 1), F32), V((1, D), F32), V((1, D), F32),
            V((2, 2, ROWS, H), BF16),
            dma((15,)), dma((NP,)), dma((NP,)), dma((2, 2, NP)), dma((2, 2, NP)), dma((NS,)), dma((NS,)), dma((16,)), dma((16,)), dma((2, 3, NP)), dma((2, 3, NP)),
            dma((4, 2, 3, NP)), dma((4, 2, 3, NP)), dma((17,)), dma((17,)),
            dma((4, 2, 3, NP)), dma((4, 2, 3, NP)), dma((3, 2, NP)), dma((3, 2, NP)), dma((4,)), dma((4,)),
        ],
        compiler_params=pltpu.CompilerParams(
            collective_id=0, has_side_effects=True, vmem_limit_bytes=61 * 1024 * 1024
        ),
        name="restore",
    )(sec, blk, act, acc, loss, gpre, wq[0], wkv[0], wo[0], gpost, tab)
    moved, newacc, check = pl.pallas_call(
        put_out,
        out_shape=(
            jax.ShapeDtypeStruct((MB, ROWS, D), BF16),
            jax.ShapeDtypeStruct((BLK, 2, D), F32),
            jax.ShapeDtypeStruct((ROWS, D), BF16),
        ),
        in_specs=[vmem] * 3,
        out_specs=(any_, any_, any_),
        scratch_shapes=[dma((3,))],
        compiler_params=pltpu.CompilerParams(vmem_limit_bytes=8 * 1024 * 1024),
        name="put_out",
    )(moved, newacc, check)
    return moved, newacc, check[None]


def solution(mesh):
    placed = (
        P("section", "dp", None),
        P(),
        P("dp", "section", None),
        P(),
        P("section", "dp"),
        P("section", None),
        P("section", None, "dp"),
        P("section", None, "dp"),
        P("section", "dp", None),
        P("section", None),
    )
    return jax.shard_map(
        on_device,
        mesh=mesh,
        in_specs=placed,
        out_specs=(P("section", "dp", None), P("dp", "section", None), P("section", "dp", None)),
        check_vma=False,
    )
```

```python
import functools

import jax
import jax.numpy as jnp
import numpy as np
from jax import lax
from jax.experimental import pallas as pl
from jax.experimental.pallas import tpu as pltpu
from jax.sharding import PartitionSpec as P

MESH = pl.DeviceIdType.MESH
D = 4608
H = D // 2
HD = 128
NS = 8
NY = 4
NZ = 4
MB = 8
ROWS = 16
BLK = 32
EPS = 1e-06
NP = 2
HP = H // NP
HW = H + 128
F32 = jnp.float32
BF16 = jnp.bfloat16

GATHER = (
    ("near", 0, 0), ("row", 0, 0, 0), ("row", 0, 1, 0), ("near", 1, 0), ("ony", 0, 0, 0),
    ("ony", 0, 1, 0), ("row", 2, 0, 0), ("row", 1, 0, 0), ("scaled", 1), ("near", 0, 1),
    ("row", 0, 0, 1), ("row", 0, 1, 1), ("near", 1, 1), ("row", 1, 1, 0), ("row", 2, 1, 0),
    ("onz", 1, 0), ("ony", 0, 0, 1), ("ony", 1, 0, 0), ("onz", 0, 1), ("ony", 0, 1, 1),
    ("onz", 0, 0), ("ony", 2, 0, 0), ("row", 1, 0, 1), ("row", 1, 1, 1), ("onz", 1, 1),
    ("row", 2, 1, 1), ("row", 2, 0, 1), ("blocks",), ("project", 0), ("ony", 1, 0, 1),
    ("row", 3, 1, 0), ("finish", 0), ("moved",), ("ony", 1, 1, 0), ("row", 3, 1, 1),
    ("ony", 1, 1, 1), ("ony", 2, 1, 0), ("ony", 2, 1, 1), ("row", 3, 0, 1), ("row", 3, 0, 0),
    ("ony", 2, 0, 1), ("relay",), ("ony", 3, 1, 0), ("ony", 3, 1, 1), ("ony", 3, 0, 0),
    ("ony", 3, 0, 1), ("project", 1), ("project", 2), ("project", 3), ("finish", 1),
    ("finish", 2), ("finish", 3),
)

REDUCE = (
    ("part", 0), ("far", 0, 0, 0), ("far", 0, 0, 1), ("part", 1), ("far", 1, 0, 0),
    ("side", 1, 1, 0), ("side", 1, 0, 0), ("attend", 3), ("own", 0, 0, 0), ("side", 1, 0, 1),
    ("side", 1, 1, 1), ("far", 0, 1, 0), ("far", 1, 1, 0), ("far", 0, 1, 1), ("middle", 0, 0, 0),
    ("far", 1, 0, 1), ("part", 2), ("own", 0, 1, 1), ("far", 2, 0, 0), ("own", 0, 1, 0),
    ("side", 2, 1, 0), ("side", 2, 1, 1), ("middle", 0, 1, 0), ("own", 0, 0, 1), ("part", 3),
    ("middle", 0, 0, 1), ("side", 2, 0, 1), ("zfar", 0, 0), ("cores",), ("middle", 0, 1, 1),
    ("side", 2, 0, 0), ("far", 2, 1, 1), ("middle", 2, 0, 0), ("middle", 1, 0, 0), ("zfar", 1, 0),
    ("far", 1, 1, 1), ("middle", 1, 0, 1), ("zfar", 0, 1), ("far", 2, 1, 0), ("middle", 1, 1, 0),
    ("zfar", 1, 1), ("middle", 2, 1, 1), ("far", 2, 0, 1), ("far", 3, 1, 1), ("far", 3, 0, 0),
    ("zmid", 0, 0), ("zown", 0, 0), ("middle", 1, 1, 1), ("middle", 2, 1, 0), ("far", 3, 1, 0),
    ("own", 3, 0, 0), ("zown", 0, 1), ("zmid", 1, 0), ("middle", 2, 0, 1), ("far", 3, 0, 1),
    ("zown", 1, 1), ("middle", 3, 0, 0), ("own", 3, 1, 1), ("own", 3, 1, 0), ("zmid", 1, 1),
    ("place",), ("middle", 3, 1, 0), ("middle", 3, 1, 1), ("zown", 1, 0), ("own", 3, 0, 1),
    ("zmid", 0, 1), ("middle", 3, 0, 1), ("finish", 1, 1), ("finish", 0, 0), ("finish", 1, 0),
    ("finish", 0, 1),
)


def rotary_tables():
    freqs = (10000.0 ** (-2.0 * np.arange(HD // 2, dtype=np.float32) / HD)).astype(np.float32)
    angles = np.arange(512, dtype=np.float32)[:, None] * freqs[None, :]
    cosine, sine = np.cos(angles), np.sin(angles)
    full = np.stack(
        [np.concatenate([cosine, cosine], axis=1), np.concatenate([-sine, sine], axis=1)]
    )
    return full.astype(np.float32).reshape(2, NY, NZ, 32, HD)


def kernel(
    sec_hbm, blk_hbm, act_hbm, acc_hbm, loss_hbm, gpre_hbm, wq_hbm, wkv_hbm, wo_hbm, gpost_hbm, tab_hbm,
    moved_v, newacc_v, checkb,
    act_v, asend, recv_a0, recv_a1, acc_v, bsend, b1, b2, b3, bre,
    lsend, lry, lsum, lrz, lfin, lrc,
    nbuf, xh, wbuf, wobuf, rbuf, rrq, rrkv, qf, kf, vf, at2,
    pbuf, yrh, yro, yrm, zrh, zro, zrm, zs, fb, finr, outb, tab, sec, blk, loss_ref, gpre, gpost,
    zrs, loc, df_s, df_r, dx_s, dx_r, a_s, a_r, bl_s, bl_r, cz_s, cz_r, cy_s, cy_r, cc_s, cc_r, dy_s, dy_r, dz_s, dz_r, bz_s, bz_r,
):
    recv_a = (recv_a0, recv_a1)
    s = lax.axis_index("section")
    d = lax.axis_index("dp")
    y = lax.div(d, 8)
    z = lax.rem(lax.div(d, 2), 4)
    c = lax.rem(d, 2)
    o = 1 - c

    def ring(v, r, n):
        return lax.rem(v + (r + n), n)

    def dp_of(yy, zz, cc):
        return (yy * NZ + zz) * 2 + cc

    at_y = {r: (s, dp_of(ring(y, r, NY), z, c)) for r in (1, 2, 3, -1)}
    at_z = {r: (s, dp_of(y, ring(z, r, NZ), c)) for r in (1, 2, 3, -1)}
    at_c = (s, dp_of(y, z, o))
    ahead = 1 - 2 * c
    ya, yb, yf = ring(y, ahead, NY), ring(y, -ahead, NY), ring(y, 2, NY)
    za, zb, zf = ring(z, ahead, NZ), ring(z, -ahead, NZ), ring(z, 2, NZ)
    to_ya, to_yb = (s, dp_of(ya, z, c)), (s, dp_of(yb, z, c))
    to_za, to_zb = (s, dp_of(y, za, c)), (s, dp_of(y, zb, c))
    at_s = {r: (ring(s, r, NS), d) for r in range(1, NS)}

    barrier = pltpu.get_barrier_semaphore()
    greet = [at_s[r] for r in range(1, NS)] + [at_y[r] for r in (1, 2, 3)]
    greet += [at_z[r] for r in (1, 2, 3)] + [at_c]
    for who in greet:
        pl.semaphore_signal(barrier, inc=1, device_id=who, device_id_type=MESH)

    pending, seen = [], set()

    def arrived(copy):
        if id(copy) not in seen:
            seen.add(id(copy))
            copy.wait_recv()

    def remote(src, dst, send_sem, recv_sem, who):
        copy = pltpu.make_async_remote_copy(
            src_ref=src, dst_ref=dst, send_sem=send_sem, recv_sem=recv_sem,
            device_id=who, device_id_type=MESH,
        )
        copy.start()
        pending.append(copy)
        return copy

    load_act = pltpu.make_async_copy(act_hbm, act_v, loc.at[0])
    load_acc = pltpu.make_async_copy(acc_hbm, acc_v, loc.at[1])
    own_rows = pl.ds(pl.multiple_of(c * H, 128), H)
    own_lanes = pl.ds(pl.multiple_of(c * HD, 128), HD)
    kv_lanes = pl.ds(pl.multiple_of(2 * HD + c * HD, 128), HD)
    other_rows = pl.ds(pl.multiple_of(o * H, 128), H)
    load_wq = pltpu.make_async_copy(wq_hbm.at[own_rows, :], wbuf.at[:, own_lanes], loc.at[2])
    load_wkv = pltpu.make_async_copy(wkv_hbm.at[own_rows, :], wbuf.at[:, kv_lanes], loc.at[3])
    load_wo = pltpu.make_async_copy(wo_hbm.at[:, own_rows], wobuf.at[c], loc.at[4])
    load_tab = pltpu.make_async_copy(tab_hbm, tab, loc.at[9])
    small = [
        pltpu.make_async_copy(source, into, loc.at[10 + i])
        for i, (source, into) in enumerate(
            ((sec_hbm, sec), (loss_hbm, loss_ref), (blk_hbm, blk), (gpre_hbm, gpre),
             (gpost_hbm, gpost))
        )
    ]
    load_act.start()
    for copy in small:
        copy.start()
    load_acc.start()
    load_wq.start()
    load_wkv.start()
    load_wo.start()
    load_tab.start()

    load_act.wait()
    small[0].wait()
    small[1].wait()
    for r in range(NS):
        to = ring(s, r, NS)
        at = jnp.int32(0)
        for j in range(MB):
            source = sec[to * MB + j]
            at = at + jnp.where((source >> 3) == s, source & 7, 0)
        chosen = act_v[at]
        for p in range(NP):
            for h in range(2):
                first = h * H + p * HP
                if r == 0:
                    recv_a[p][s, h] = chosen[:, first : first + HP]
                else:
                    asend[r, p, h] = chosen[:, first : first + HP]
    lsend[...] = jnp.broadcast_to(loss_ref[...], (1, HD))

    pl.semaphore_wait(barrier, len(greet))

    from_s = {}
    for p in range(NP):
        for r in range(1, NS):
            from_s[p, r] = remote(
                asend.at[r, p], recv_a[p].at[s], a_s.at[r, p], a_r.at[r, p], at_s[r]
            )
    from_ly = [
        remote(lsend, lry.at[r], bl_s.at[8 + r], bl_r.at[8 + r], at_y[r]) for r in (1, 2, 3)
    ]
    w_q = remote(wq_hbm.at[other_rows, :], wbuf.at[:, own_lanes], cc_s.at[0], cc_r.at[0], at_c)
    w_kv = remote(wkv_hbm.at[other_rows, :], wbuf.at[:, kv_lanes], cc_s.at[1], cc_r.at[1], at_c)
    w_o = remote(wo_hbm.at[:, other_rows], wobuf.at[c], cc_s.at[2], cc_r.at[2], at_c)

    load_acc.wait()
    for copy in small[2:]:
        copy.wait()
    from_by = []
    for r in (1, 2, 3, 0):
        base = ring(y, r, NY) * 8

        def pick(k, carry, r=r, base=base):
            first = (base + k) * BLK
            at = jnp.int32(0)
            for b in range(BLK):
                source = blk[first + b]
                at = at + jnp.where((source >> 5) == d, source & 31, 0)
            into = b1.at[0] if r == 0 else bsend.at[r]
            into[lax.div(k, 2), lax.rem(k, 2)] = acc_v[at].astype(BF16)
            return carry

        lax.fori_loop(0, 8, pick, 0)
        if r:
            from_by.append(
                remote(bsend.at[r], b1.at[r], bl_s.at[r], bl_r.at[r], at_y[r])
            )

    def lanes(p):
        return pl.ds(p * HP, HP if p < NP - 1 else HW - p * HP)

    squares, core_n = [], {}

    def do_scaled(p):
        for r in range(1, NS):
            from_s[p, r].wait_recv()
        x = recv_a[p][sec[s * MB] >> 3]
        for h in range(2):
            xf = x[h].astype(F32)
            squares.append(jnp.sum(xf * xf, axis=-1, keepdims=True))
            first = h * H + p * HP
            nbuf[h, :, p * HP : (p + 1) * HP] = (xf * gpre[:, first : first + HP]).astype(BF16)
        if p == NP - 1:
            scale = lax.rsqrt(sum(squares) / D + EPS)
            high_part = scale.astype(BF16).astype(F32)
            lane = lax.broadcasted_iota(jnp.int32, (ROWS, 128), 1)
            both = jnp.where(lane < 64, high_part, scale - high_part).astype(BF16)
            nbuf[0, :, H:] = both
            nbuf[1, :, H:] = both
        xh[y, z, c, :, lanes(p)] = nbuf[c, :, lanes(p)]
        core_n[p] = remote(
            nbuf.at[o, :, lanes(p)], xh.at[y, z, c, :, lanes(p)],
            df_s.at[NP + p], df_r.at[NP + p], at_c,
        )

    do_scaled(0)
    half = (c, o)

    def piece_of(yy, zz, i, p):
        return xh.at[yy, zz, half[i], :, lanes(p)]

    order = [z, zb, za, zf]
    near_z, far_z, rows_y, rows_on = {}, {}, {}, {}

    def do_near(i, p):
        piece = piece_of(y, z, i, p)
        for way, who in enumerate((to_za, to_zb)):
            near_z[i, p, way] = remote(
                piece, piece, cz_s.at[i, way, p], cz_r.at[i, way, p], who
            )

    def do_row(q, i, p):
        if q == 1 or q == 2:
            arrived(near_z[i, p, q - 1])
        if q == 3:
            far_z[i, p].wait_recv()
        piece = piece_of(y, order[q], i, p)
        for way, who in enumerate((to_ya, to_yb)):
            rows_y[q, i, p, way] = remote(
                piece, piece, cy_s.at[q, i, way, p], cy_r.at[q, i, way, p], who
            )

    def do_onz(i, p):
        arrived(near_z[i, p, i])
        piece = piece_of(y, (zb, za)[i], i, p)
        far_z[i, p] = remote(
            piece, piece, cz_s.at[i, 2, p], cz_r.at[i, 2, p], (to_za, to_zb)[i]
        )

    def do_ony(q, i, p):
        rows_y[q, i, p, i].wait_recv()
        piece = piece_of((yb, ya)[i], order[q], i, p)
        rows_on[q, i, p] = remote(
            piece, piece, cy_s.at[q, i, 2, p], cy_r.at[q, i, 2, p], (to_ya, to_yb)[i]
        )

    def do_project(q):
        if q == 0:
            load_tab.wait()
            load_wq.wait()
            load_wkv.wait()
            w_q.wait_recv()
            w_kv.wait_recv()
        zz = order[q]
        for i in range(2):
            for p in range(NP):
                rows_y[q, i, p, 1 - i].wait_recv()
                rows_on[q, i, p].wait_recv()
        rows = xh[:, zz, :, :, 0:H].reshape(128, H)
        res = jnp.dot(rows, wbuf[...], preferred_element_type=F32)
        for j in range(4):
            rbuf[q, j] = res[:, j * HD : (j + 1) * HD]
        shared[q] = [
            remote(rbuf.at[q, o], rrq.at[zz], cc_s.at[4 + zz], cc_r.at[4 + zz], at_c),
            remote(rbuf.at[q, pl.ds(2, 2)], rrkv.at[zz], cc_s.at[8 + zz], cc_r.at[8 + zz], at_c),
        ]

    def do_finish(q):
        zz = order[q]
        for copy in shared[q]:
            copy.wait_recv()
        cosine = tab[0, :, zz].reshape(128, HD)
        sine = tab[1, :, zz].reshape(128, HD)
        parts = xh[:, zz, :, :, H:HW].reshape(128, 128).astype(F32)
        scale = parts[:, 0:1] + parts[:, 64:65]
        query = (rbuf[q, c] + rrq[zz]) * scale
        key = (rbuf[q, 2] + rrkv[zz, 0]) * scale
        value = (rbuf[q, 3] + rrkv[zz, 1]) * scale
        query = query * cosine + pltpu.roll(query, HD // 2, 1) * sine
        key = key * cosine + pltpu.roll(key, HD // 2, 1) * sine
        qf[:, zz] = query.astype(BF16).reshape(NY, 32, HD)
        kf[:, zz] = key.astype(BF16).reshape(NY, 32, HD)
        vf[:, zz] = value.astype(BF16).reshape(NY, 32, HD)

    shared, relay, from_lz, from_bz = {}, [], [], []
    low, high = pl.ds(0, 2), pl.ds(2, 2)

    def do_blocks():
        for copy in from_ly:
            copy.wait_recv()
        lsum[...] = lsend[...] + lry[1] + lry[2] + lry[3]
        from_lz.extend(
            remote(lsum, lrz.at[r], bl_s.at[11 + r], bl_r.at[11 + r], at_z[r])
            for r in (1, 2, 3)
        )
        for copy in from_by:
            copy.wait_recv()
        b_far = b1.at[:, ring(z, 2, NZ)]
        relay.append(remote(b_far.at[low], bre.at[0], bz_s.at[0], bz_r.at[0], at_z[1]))
        relay.append(remote(b_far.at[high], bre.at[1], bz_s.at[1], bz_r.at[1], at_z[-1]))
        for r in (1, 3):
            from_bz.append(
                remote(b1.at[:, ring(z, r, NZ)], b2.at[r], bl_s.at[3 + r], bl_r.at[3 + r], at_z[r])
            )
        b2[0] = b1[:, z]

    def do_relay():
        for i, (part_of, who) in enumerate(((low, at_z[1]), (high, at_z[-1]))):
            relay[i].wait_recv()
            from_bz.append(
                remote(bre.at[i], b2.at[2, part_of], bz_s.at[2 + i], bz_r.at[2 + i], who)
            )

    def do_moved():
        for j in range(MB):
            for p in range(NP):
                rows = recv_a[p][sec[s * MB + j] >> 3]
                for h in range(2):
                    moved_v[j, :, h * H + p * HP : h * H + (p + 1) * HP] = rows[h]

    steps = dict(
        near=do_near, row=do_row, onz=do_onz, ony=do_ony, project=do_project,
        finish=do_finish, blocks=do_blocks, relay=do_relay, moved=do_moved,
        scaled=do_scaled,
    )
    for name, *which in GATHER:
        if (name == "near" or (name == "row" and which[0] == 0)) and which[-2] == 1:
            if which[-1] in core_n:
                core_n.pop(which[-1]).wait_recv()
        with jax.named_scope("_".join([name] + [str(w) for w in which])):
            steps[name](*which)
    back = [zf, zb, za, z]
    keys, values = kf[...].reshape(512, HD), vf[...].reshape(512, HD)
    line = lax.broadcasted_iota(jnp.int32, (128, 512), 0)
    token = ((line >> 5) << 7) + (line & 31)
    col = lax.broadcasted_iota(jnp.int32, (128, 512), 1)
    from_att = {}

    def do_attend(m):
        scores = lax.dot_general(
            qf[:, back[m]].reshape(128, HD), keys,
            (((1,), (1,)), ((), ())), preferred_element_type=F32,
        ) * ((D / 32) ** (-0.5))
        capped = 50.0 * jnp.tanh(scores / 50.0)
        expd = jnp.where(col <= token + back[m] * 32, jnp.exp(capped), 0.0)
        total = jnp.sum(expd, axis=-1, keepdims=True)
        numer = jnp.dot(expd.astype(BF16), values, preferred_element_type=F32)
        zz = back[m]
        at2[c, zz] = (numer / total).astype(BF16)
        from_att[m] = remote(
            at2.at[c, zz], at2.at[c, zz], cc_s.at[12 + zz], cc_r.at[12 + zz], at_c
        )

    for m in range(3):
        do_attend(m)

    y_far, y_own, y_mid, z_side, z_far, z_own, z_mid, late = {}, {}, {}, {}, {}, {}, {}, {}

    def cols(p):
        return pl.ds(p * HP, HP)

    def mine_at(yy, q, i, p):
        return pbuf.at[yy, back[q], half[i], :, cols(p)]

    def do_part(q):
        if q == 0:
            load_wo.wait()
            w_o.wait_recv()
        from_att[q].wait_recv()
        res = jnp.dot(at2[0, back[q]], wobuf[0], preferred_element_type=F32)
        res = res + jnp.dot(at2[1, back[q]], wobuf[1], preferred_element_type=F32)
        pbuf[:, back[q]] = res.astype(BF16).reshape(NY, 2, ROWS, H)

    def do_far(q, i, p):
        y_far[q, i, p] = remote(
            mine_at(yf, q, i, p), yrh.at[q, i, :, cols(p)],
            dy_s.at[q, i, 0, p], dy_r.at[q, i, 0, p], (to_ya, to_yb)[i],
        )

    def do_own(q, i, p):
        source = mine_at((yb, ya)[i], q, i, p)
        if q == 3:
            z_side[1, i, p].wait_recv()
            z_side[2, i, p].wait_recv()
            total = source[...].astype(F32) + zrs[0, i, :, cols(p)].astype(F32)
            source[...] = (total + zrs[1, i, :, cols(p)].astype(F32)).astype(BF16)
        y_own[q, i, p] = remote(
            source, yro.at[q, i, :, cols(p)],
            dy_s.at[q, i, 1, p], dy_r.at[q, i, 1, p], (to_yb, to_ya)[i],
        )

    def do_side(q, i, p):
        z_side[q, i, p] = remote(
            mine_at((yb, ya)[i], q, i, p), zrs.at[q - 1, i, :, cols(p)],
            dx_s.at[q - 1, i, p], dx_r.at[q - 1, i, p], (to_zb, to_za)[q - 1],
        )

    def do_middle(q, i, p):
        y_far[q, i, p].wait_recv()
        source = mine_at((ya, yb)[i], q, i, p)
        total = source[...].astype(F32) + yrh[q, i, :, cols(p)].astype(F32)
        source[...] = total.astype(BF16)
        y_mid[q, i, p] = remote(
            source, yrm.at[q, i, :, cols(p)],
            dy_s.at[q, i, 2, p], dy_r.at[q, i, 2, p], (to_ya, to_yb)[i],
        )

    def reduced(q, i, p):
        total = mine_at(y, q, i, p)[...].astype(F32)
        if q == 0 or q == 3:
            y_own[q, i, p].wait_recv()
            total = total + yro[q, i, :, cols(p)].astype(F32)
        y_mid[q, i, p].wait_recv()
        return total + yrm[q, i, :, cols(p)].astype(F32)

    def send_z(value, kind, i, p, into, who):
        zs[kind, i, :, cols(p)] = value.astype(BF16)
        return remote(
            zs.at[kind, i, :, cols(p)], into.at[i, :, cols(p)],
            dz_s.at[kind, i, p], dz_r.at[kind, i, p], who,
        )

    def do_zfar(i, p):
        z_far[i, p] = send_z(reduced(0, i, p), 0, i, p, zrh, (to_za, to_zb)[i])

    def do_zown(i, p):
        z_own[i, p] = send_z(reduced(1 + i, i, p), 1, i, p, zro, (to_zb, to_za)[i])

    def do_zmid(i, p):
        total = reduced(2 - i, i, p)
        z_far[i, p].wait_recv()
        total = total + zrh[i, :, cols(p)].astype(F32)
        z_mid[i, p] = send_z(total, 2, i, p, zrm, (to_za, to_zb)[i])

    def do_cores():
        for copy in from_bz + from_lz:
            copy.wait_recv()
        late["blocks"] = remote(b2.at[:, :, o], b3, bl_s.at[7], bl_r.at[7], at_c)
        lfin[...] = lsum[...] + lrz[1] + lrz[2] + lrz[3]
        late["loss"] = remote(lfin, lrc, bl_s.at[15], bl_r.at[15], at_c)

    def do_place():
        late["loss"].wait_recv()
        late["blocks"].wait_recv()
        factor = 32.0 / (lfin[...] + lrc[...])[0, 0]

        def place(b, carry):
            source = blk[d * BLK + b] >> 5
            ry = (y - (source >> 3)) & 3
            rz = (z - ((source >> 1) & 3)) & 3
            mine = b2[rz, ry, c].astype(F32)
            theirs = b3[rz, ry].astype(F32)
            newacc_v[b] = jnp.where((source & 1) == c, mine, theirs) * factor
            return carry

        lax.fori_loop(0, BLK, place, 0)

    def do_finish_sum(i, p):
        total = reduced(3, i, p)
        z_own[i, p].wait_recv()
        z_mid[i, p].wait_recv()
        total = total + zro[i, :, cols(p)].astype(F32)
        fb[i, :, cols(p)] = total + zrm[i, :, cols(p)].astype(F32)
        if i == 1:
            late[p] = remote(
                fb.at[1, :, cols(p)], finr.at[:, cols(p)], df_s.at[p], df_r.at[p], at_c
            )

    steps = dict(
        part=do_part, far=do_far, own=do_own, side=do_side, middle=do_middle, zfar=do_zfar,
        zown=do_zown, zmid=do_zmid, cores=do_cores, place=do_place, finish=do_finish_sum,
        attend=do_attend,
    )
    for name, *which in REDUCE:
        with jax.named_scope("_".join([name] + [str(w) for w in which])):
            steps[name](*which)
    checked = [recv_a[p][sec[s * MB] >> 3].astype(F32) for p in range(NP)]
    for p in range(NP):
        late[p].wait_recv()
    mine = fb[0]
    theirs = finr[...]
    meansq = jnp.sum(mine * mine, axis=-1, keepdims=True)
    meansq = (meansq + jnp.sum(theirs * theirs, axis=-1, keepdims=True)) / D
    scale = lax.rsqrt(meansq + EPS)
    outb[c] = mine
    outb[o] = theirs
    for h in range(2):
        for p in range(NP):
            cols_of = slice(h * H + p * HP, h * H + (p + 1) * HP)
            change = outb[h, :, p * HP : (p + 1) * HP] * scale * gpost[:, cols_of]
            checkb[:, cols_of] = (checked[p][h] + change).astype(BF16)
    for copy in pending:
        copy.wait_send()


def put_out(moved, newacc, check, moved_hbm, newacc_hbm, check_hbm, sem):
    copies = [
        pltpu.make_async_copy(source, into, sem.at[i])
        for i, (source, into) in enumerate(
            ((newacc, newacc_hbm), (moved, moved_hbm), (check, check_hbm))
        )
    ]
    for copy in copies:
        copy.start()
    for copy in copies:
        copy.wait()


def on_device(act, sec, acc, blk, loss, gpre, wq, wkv, wo, gpost):
    tab = jnp.asarray(rotary_tables())
    any_ = pl.BlockSpec(memory_space=pl.ANY)
    vmem = pl.BlockSpec(memory_space=pltpu.VMEM)
    V = pltpu.VMEM
    dma = pltpu.SemaphoreType.DMA
    moved, newacc, check = pl.pallas_call(
        kernel,
        out_shape=(
            V((MB, ROWS, D), BF16),
            V((BLK, 2, D), F32),
            V((ROWS, D), BF16),
        ),
        in_specs=[pl.BlockSpec(memory_space=pltpu.HBM)] * 11,
        out_specs=(vmem, vmem, vmem),
        scratch_shapes=[
            V((MB, ROWS, D), BF16), V((NS, NP, 2, ROWS, HP), BF16),
            V((NS, 2, ROWS, HP), BF16), V((NS, 2, ROWS, HP), BF16),
            V((BLK, 2, D), F32),
            V((NY, NZ, 2, 2, D), BF16), V((NY, NZ, 2, 2, D), BF16),
            V((NZ, NY, 2, 2, D), BF16), V((NZ, NY, 2, D), BF16), V((2, 2, 2, 2, D), BF16),
            V((1, HD), F32), V((4, 1, HD), F32), V((1, HD), F32), V((4, 1, HD), F32),
            V((1, HD), F32), V((1, HD), F32),
            V((2, ROWS, HW), BF16), V((NY, NZ, 2, ROWS, HW), BF16), V((H, 4 * HD), BF16),
            V((2, HD, H), BF16), V((4, 4, 128, HD), F32), V((4, 128, HD), F32),
            V((4, 2, 128, HD), F32), V((NY, NZ, 32, HD), BF16), V((NY, NZ, 32, HD), BF16),
            V((NY, NZ, 32, HD), BF16), V((2, 4, 128, HD), BF16),
            V((NY, NZ, 2, ROWS, H), BF16), V((4, 2, ROWS, H), BF16), V((4, 2, ROWS, H), BF16),
            V((4, 2, ROWS, H), BF16), V((2, ROWS, H), BF16), V((2, ROWS, H), BF16),
            V((2, ROWS, H), BF16), V((3, 2, ROWS, H), BF16), V((2, ROWS, H), F32),
            V((ROWS, H), F32), V((2, ROWS, H), F32),
            V((2, NY, NZ, 32, HD), F32), pltpu.SMEM((64,), jnp.int32),
            pltpu.SMEM((1024,), jnp.int32), V((1, 1), F32), V((1, D), F32), V((1, D), F32),
            V((2, 2, ROWS, H), BF16),
            dma((15,)), dma((2 * NP,)), dma((2 * NP,)), dma((2, 2, NP)), dma((2, 2, NP)), dma((NS, NP)), dma((NS, NP)), dma((16,)), dma((16,)), dma((2, 3, NP)), dma((2, 3, NP)),
            dma((4, 2, 3, NP)), dma((4, 2, 3, NP)), dma((17,)), dma((17,)),
            dma((4, 2, 3, NP)), dma((4, 2, 3, NP)), dma((3, 2, NP)), dma((3, 2, NP)), dma((4,)), dma((4,)),
        ],
        compiler_params=pltpu.CompilerParams(
            collective_id=0, has_side_effects=True, vmem_limit_bytes=61 * 1024 * 1024
        ),
        name="restore",
    )(sec, blk, act, acc, loss, gpre, wq[0], wkv[0], wo[0], gpost, tab)
    moved, newacc, check = pl.pallas_call(
        put_out,
        out_shape=(
            jax.ShapeDtypeStruct((MB, ROWS, D), BF16),
            jax.ShapeDtypeStruct((BLK, 2, D), F32),
            jax.ShapeDtypeStruct((ROWS, D), BF16),
        ),
        in_specs=[vmem] * 3,
        out_specs=(any_, any_, any_),
        scratch_shapes=[dma((3,))],
        compiler_params=pltpu.CompilerParams(vmem_limit_bytes=8 * 1024 * 1024),
        name="put_out",
    )(moved, newacc, check)
    return moved, newacc, check[None]


def solution(mesh):
    placed = (
        P("section", "dp", None),
        P(),
        P("dp", "section", None),
        P(),
        P("section", "dp"),
        P("section", None),
        P("section", None, "dp"),
        P("section", None, "dp"),
        P("section", "dp", None),
        P("section", None),
    )
    return jax.shard_map(
        on_device,
        mesh=mesh,
        in_specs=placed,
        out_specs=(P("section", "dp", None), P("dp", "section", None), P("section", "dp", None)),
        check_vma=False,
    )
```

```python
import functools

import jax
import jax.numpy as jnp
import numpy as np
from jax import lax
from jax.experimental import pallas as pl
from jax.experimental.pallas import tpu as pltpu
from jax.sharding import PartitionSpec as P

MESH = pl.DeviceIdType.MESH
D = 4608
H = D // 2
HD = 128
NS = 8
NY = 4
NZ = 4
MB = 8
ROWS = 16
BLK = 32
EPS = 1e-06
NP = 2
HP = H // NP
HW = H + 128
F32 = jnp.float32
BF16 = jnp.bfloat16

GATHER = (
    ("near", 0, 0), ("row", 0, 0, 0), ("row", 0, 1, 0), ("near", 1, 0), ("ony", 0, 0, 0),
    ("ony", 0, 1, 0), ("row", 2, 0, 0), ("row", 1, 0, 0), ("scaled", 1), ("near", 0, 1),
    ("row", 0, 0, 1), ("row", 0, 1, 1), ("near", 1, 1), ("row", 1, 1, 0), ("row", 2, 1, 0),
    ("onz", 1, 0), ("ony", 0, 0, 1), ("ony", 1, 0, 0), ("onz", 0, 1), ("ony", 0, 1, 1),
    ("onz", 0, 0), ("ony", 2, 0, 0), ("row", 1, 0, 1), ("row", 1, 1, 1), ("onz", 1, 1),
    ("row", 2, 1, 1), ("row", 2, 0, 1), ("blocks",), ("ony", 1, 0, 1), ("row", 3, 1, 0),
    ("moved",), ("ony", 1, 1, 0), ("row", 3, 1, 1), ("ony", 1, 1, 1), ("ony", 2, 1, 0),
    ("ony", 2, 1, 1), ("row", 3, 0, 1), ("row", 3, 0, 0), ("ony", 2, 0, 1), ("ony", 3, 1, 0),
    ("ony", 3, 1, 1), ("project", 0), ("ony", 3, 0, 0), ("ony", 3, 0, 1), ("project", 1),
    ("project", 2), ("finish", 0), ("project", 3), ("finish", 1), ("finish", 2), ("finish", 3),
    ("relay",),
)

REDUCE = (
    ("attend", 1), ("part", 0), ("far", 0, 0, 0), ("far", 0, 0, 1), ("own", 0, 1, 0),
    ("own", 0, 1, 1), ("far", 0, 1, 0), ("far", 0, 1, 1), ("own", 0, 0, 0), ("own", 0, 0, 1),
    ("attend", 2), ("part", 1), ("far", 1, 0, 0), ("side", 1, 1, 0), ("side", 1, 0, 0),
    ("attend", 3), ("side", 1, 0, 1), ("side", 1, 1, 1), ("far", 1, 1, 0), ("middle", 0, 0, 0),
    ("far", 1, 0, 1), ("part", 2), ("far", 2, 0, 0), ("side", 2, 1, 0), ("side", 2, 1, 1),
    ("middle", 0, 1, 0), ("part", 3), ("middle", 0, 0, 1), ("side", 2, 0, 1), ("zfar", 0, 0),
    ("middle", 0, 1, 1), ("side", 2, 0, 0), ("far", 2, 1, 1), ("middle", 2, 0, 0),
    ("middle", 1, 0, 0), ("zfar", 1, 0), ("far", 1, 1, 1), ("middle", 1, 0, 1), ("zfar", 0, 1),
    ("far", 2, 1, 0), ("middle", 1, 1, 0), ("zfar", 1, 1), ("middle", 2, 1, 1), ("far", 2, 0, 1),
    ("far", 3, 1, 1), ("far", 3, 0, 0), ("zown", 0, 0), ("middle", 1, 1, 1), ("middle", 2, 1, 0),
    ("far", 3, 1, 0), ("own", 3, 0, 0), ("zown", 0, 1), ("zmid", 1, 0), ("cores",),
    ("zmid", 0, 0), ("middle", 2, 0, 1), ("far", 3, 0, 1), ("zown", 1, 1), ("middle", 3, 0, 0),
    ("own", 3, 1, 1), ("own", 3, 1, 0), ("zmid", 1, 1), ("middle", 3, 1, 0), ("middle", 3, 1, 1),
    ("zown", 1, 0), ("own", 3, 0, 1), ("zmid", 0, 1), ("middle", 3, 0, 1), ("place",),
    ("finish", 1, 1), ("finish", 0, 0), ("finish", 1, 0), ("finish", 0, 1),
)


def rotary_tables():
    freqs = (10000.0 ** (-2.0 * np.arange(HD // 2, dtype=np.float32) / HD)).astype(np.float32)
    angles = np.arange(512, dtype=np.float32)[:, None] * freqs[None, :]
    cosine, sine = np.cos(angles), np.sin(angles)
    full = np.stack(
        [np.concatenate([cosine, cosine], axis=1), np.concatenate([-sine, sine], axis=1)]
    )
    return full.astype(np.float32).reshape(2, NY, NZ, 32, HD)


def kernel(
    sec_hbm, blk_hbm, act_hbm, acc_hbm, loss_hbm, gpre_hbm, wq_hbm, wkv_hbm, wo_hbm, gpost_hbm, tab_hbm,
    moved_v, newacc_v, checkb,
    act_v, asend, recv_a0, recv_a1, acc_v, bsend, b1, b2, b3, bre,
    lsend, lry, lsum, lrz, lfin, lrc,
    nbuf, xh, wbuf, wobuf, rbuf, rrq, rrkv, qf, kf, vf, at2,
    pbuf, yrh, yro, yrm, zrh, zro, zrm, zs, fb, finr, outb, tab, sec, blk, loss_ref, gpre, gpost,
    zrs, loc, df_s, df_r, dx_s, dx_r, a_s, a_r, bl_s, bl_r, cz_s, cz_r, cy_s, cy_r, cc_s, cc_r, dy_s, dy_r, dz_s, dz_r, bz_s, bz_r,
):
    recv_a = (recv_a0, recv_a1)
    s = lax.axis_index("section")
    d = lax.axis_index("dp")
    y = lax.div(d, 8)
    z = lax.rem(lax.div(d, 2), 4)
    c = lax.rem(d, 2)
    o = 1 - c

    def ring(v, r, n):
        return lax.rem(v + (r + n), n)

    def dp_of(yy, zz, cc):
        return (yy * NZ + zz) * 2 + cc

    at_y = {r: (s, dp_of(ring(y, r, NY), z, c)) for r in (1, 2, 3, -1)}
    at_z = {r: (s, dp_of(y, ring(z, r, NZ), c)) for r in (1, 2, 3, -1)}
    at_c = (s, dp_of(y, z, o))
    ahead = 1 - 2 * c
    ya, yb, yf = ring(y, ahead, NY), ring(y, -ahead, NY), ring(y, 2, NY)
    za, zb, zf = ring(z, ahead, NZ), ring(z, -ahead, NZ), ring(z, 2, NZ)
    to_ya, to_yb = (s, dp_of(ya, z, c)), (s, dp_of(yb, z, c))
    to_za, to_zb = (s, dp_of(y, za, c)), (s, dp_of(y, zb, c))
    at_s = {r: (ring(s, r, NS), d) for r in range(1, NS)}

    barrier = pltpu.get_barrier_semaphore()
    greet = [at_s[r] for r in range(1, NS)] + [at_y[r] for r in (1, 2, 3)]
    greet += [at_z[r] for r in (1, 2, 3)] + [at_c]
    for who in greet:
        pl.semaphore_signal(barrier, inc=1, device_id=who, device_id_type=MESH)

    pending, seen = [], set()

    def arrived(copy):
        if id(copy) not in seen:
            seen.add(id(copy))
            copy.wait_recv()

    def remote(src, dst, send_sem, recv_sem, who):
        copy = pltpu.make_async_remote_copy(
            src_ref=src, dst_ref=dst, send_sem=send_sem, recv_sem=recv_sem,
            device_id=who, device_id_type=MESH,
        )
        copy.start()
        pending.append(copy)
        return copy

    load_act = pltpu.make_async_copy(act_hbm, act_v, loc.at[0])
    load_acc = pltpu.make_async_copy(acc_hbm, acc_v, loc.at[1])
    own_rows = pl.ds(pl.multiple_of(c * H, 128), H)
    own_lanes = pl.ds(pl.multiple_of(c * HD, 128), HD)
    kv_lanes = pl.ds(pl.multiple_of(2 * HD + c * HD, 128), HD)
    other_rows = pl.ds(pl.multiple_of(o * H, 128), H)
    load_wq = pltpu.make_async_copy(wq_hbm.at[own_rows, :], wbuf.at[:, own_lanes], loc.at[2])
    load_wkv = pltpu.make_async_copy(wkv_hbm.at[own_rows, :], wbuf.at[:, kv_lanes], loc.at[3])
    load_wo = pltpu.make_async_copy(wo_hbm.at[:, own_rows], wobuf.at[c], loc.at[4])
    load_tab = pltpu.make_async_copy(tab_hbm, tab, loc.at[9])
    small = [
        pltpu.make_async_copy(source, into, loc.at[10 + i])
        for i, (source, into) in enumerate(
            ((sec_hbm, sec), (loss_hbm, loss_ref), (blk_hbm, blk), (gpre_hbm, gpre),
             (gpost_hbm, gpost))
        )
    ]
    load_act.start()
    for copy in small:
        copy.start()
    load_acc.start()
    load_wq.start()
    load_wkv.start()
    load_wo.start()
    load_tab.start()

    load_act.wait()
    small[0].wait()
    small[1].wait()
    for r in range(NS):
        to = ring(s, r, NS)
        at = jnp.int32(0)
        for j in range(MB):
            source = sec[to * MB + j]
            at = at + jnp.where((source >> 3) == s, source & 7, 0)
        chosen = act_v[at]
        for p in range(NP):
            for h in range(2):
                first = h * H + p * HP
                if r == 0:
                    recv_a[p][s, h] = chosen[:, first : first + HP]
                else:
                    asend[r, p, h] = chosen[:, first : first + HP]
    lsend[...] = jnp.broadcast_to(loss_ref[...], (1, HD))

    pl.semaphore_wait(barrier, len(greet))

    from_s = {}
    for p in range(NP):
        for r in range(1, NS):
            from_s[p, r] = remote(
                asend.at[r, p], recv_a[p].at[s], a_s.at[r, p], a_r.at[r, p], at_s[r]
            )
    from_ly = [
        remote(lsend, lry.at[r], bl_s.at[8 + r], bl_r.at[8 + r], at_y[r]) for r in (1, 2, 3)
    ]
    w_q = remote(wq_hbm.at[other_rows, :], wbuf.at[:, own_lanes], cc_s.at[0], cc_r.at[0], at_c)
    w_kv = remote(wkv_hbm.at[other_rows, :], wbuf.at[:, kv_lanes], cc_s.at[1], cc_r.at[1], at_c)
    w_o = remote(wo_hbm.at[:, other_rows], wobuf.at[c], cc_s.at[2], cc_r.at[2], at_c)

    load_acc.wait()
    for copy in small[2:]:
        copy.wait()
    from_by = []
    for r in (1, 2, 3, 0):
        base = ring(y, r, NY) * 8

        def pick(k, carry, r=r, base=base):
            first = (base + k) * BLK
            at = jnp.int32(0)
            for b in range(BLK):
                source = blk[first + b]
                at = at + jnp.where((source >> 5) == d, source & 31, 0)
            into = b1.at[0] if r == 0 else bsend.at[r]
            into[lax.div(k, 2), lax.rem(k, 2)] = acc_v[at].astype(BF16)
            return carry

        lax.fori_loop(0, 8, pick, 0)
        if r:
            from_by.append(
                remote(bsend.at[r], b1.at[r], bl_s.at[r], bl_r.at[r], at_y[r])
            )

    def lanes(p):
        return pl.ds(p * HP, HP if p < NP - 1 else HW - p * HP)

    squares, core_n = [], {}

    def do_scaled(p):
        for r in range(1, NS):
            from_s[p, r].wait_recv()
        x = recv_a[p][sec[s * MB] >> 3]
        for h in range(2):
            xf = x[h].astype(F32)
            squares.append(jnp.sum(xf * xf, axis=-1, keepdims=True))
            first = h * H + p * HP
            nbuf[h, :, p * HP : (p + 1) * HP] = (xf * gpre[:, first : first + HP]).astype(BF16)
        if p == NP - 1:
            scale = lax.rsqrt(sum(squares) / D + EPS)
            high_part = scale.astype(BF16).astype(F32)
            lane = lax.broadcasted_iota(jnp.int32, (ROWS, 128), 1)
            both = jnp.where(lane < 64, high_part, scale - high_part).astype(BF16)
            nbuf[0, :, H:] = both
            nbuf[1, :, H:] = both
        xh[y, z, c, :, lanes(p)] = nbuf[c, :, lanes(p)]
        core_n[p] = remote(
            nbuf.at[o, :, lanes(p)], xh.at[y, z, c, :, lanes(p)],
            df_s.at[NP + p], df_r.at[NP + p], at_c,
        )

    do_scaled(0)
    half = (c, o)

    def piece_of(yy, zz, i, p):
        return xh.at[yy, zz, half[i], :, lanes(p)]

    order = [z, zb, za, zf]
    near_z, far_z, rows_y, rows_on = {}, {}, {}, {}

    def do_near(i, p):
        piece = piece_of(y, z, i, p)
        for way, who in enumerate((to_za, to_zb)):
            near_z[i, p, way] = remote(
                piece, piece, cz_s.at[i, way, p], cz_r.at[i, way, p], who
            )

    def do_row(q, i, p):
        if q == 1 or q == 2:
            arrived(near_z[i, p, q - 1])
        if q == 3:
            far_z[i, p].wait_recv()
        piece = piece_of(y, order[q], i, p)
        for way, who in enumerate((to_ya, to_yb)):
            rows_y[q, i, p, way] = remote(
                piece, piece, cy_s.at[q, i, way, p], cy_r.at[q, i, way, p], who
            )

    def do_onz(i, p):
        arrived(near_z[i, p, i])
        piece = piece_of(y, (zb, za)[i], i, p)
        far_z[i, p] = remote(
            piece, piece, cz_s.at[i, 2, p], cz_r.at[i, 2, p], (to_za, to_zb)[i]
        )

    def do_ony(q, i, p):
        rows_y[q, i, p, i].wait_recv()
        piece = piece_of((yb, ya)[i], order[q], i, p)
        rows_on[q, i, p] = remote(
            piece, piece, cy_s.at[q, i, 2, p], cy_r.at[q, i, 2, p], (to_ya, to_yb)[i]
        )

    def do_project(q):
        if q == 0:
            load_tab.wait()
            load_wq.wait()
            load_wkv.wait()
            w_q.wait_recv()
            w_kv.wait_recv()
        zz = order[q]
        for i in range(2):
            for p in range(NP):
                rows_y[q, i, p, 1 - i].wait_recv()
                rows_on[q, i, p].wait_recv()
        rows = xh[:, zz, :, :, 0:H].reshape(128, H)
        res = jnp.dot(rows, wbuf[...], preferred_element_type=F32)
        for j in range(4):
            rbuf[q, j] = res[:, j * HD : (j + 1) * HD]
        shared[q] = [
            remote(rbuf.at[q, o], rrq.at[zz], cc_s.at[4 + zz], cc_r.at[4 + zz], at_c),
            remote(rbuf.at[q, pl.ds(2, 2)], rrkv.at[zz], cc_s.at[8 + zz], cc_r.at[8 + zz], at_c),
        ]

    def do_finish(q):
        zz = order[q]
        for copy in shared[q]:
            copy.wait_recv()
        cosine = tab[0, :, zz].reshape(128, HD)
        sine = tab[1, :, zz].reshape(128, HD)
        parts = xh[:, zz, :, :, H:HW].reshape(128, 128).astype(F32)
        scale = parts[:, 0:1] + parts[:, 64:65]
        query = (rbuf[q, c] + rrq[zz]) * scale
        key = (rbuf[q, 2] + rrkv[zz, 0]) * scale
        value = (rbuf[q, 3] + rrkv[zz, 1]) * scale
        query = query * cosine + pltpu.roll(query, HD // 2, 1) * sine
        key = key * cosine + pltpu.roll(key, HD // 2, 1) * sine
        qf[:, zz] = query.astype(BF16).reshape(NY, 32, HD)
        kf[:, zz] = key.astype(BF16).reshape(NY, 32, HD)
        vf[:, zz] = value.astype(BF16).reshape(NY, 32, HD)

    shared, relay, from_lz, from_bz = {}, [], [], []
    low, high = pl.ds(0, 2), pl.ds(2, 2)

    def do_blocks():
        for copy in from_ly:
            copy.wait_recv()
        lsum[...] = lsend[...] + lry[1] + lry[2] + lry[3]
        from_lz.extend(
            remote(lsum, lrz.at[r], bl_s.at[11 + r], bl_r.at[11 + r], at_z[r])
            for r in (1, 2, 3)
        )
        for copy in from_by:
            copy.wait_recv()
        b_far = b1.at[:, ring(z, 2, NZ)]
        relay.append(remote(b_far.at[low], bre.at[0], bz_s.at[0], bz_r.at[0], at_z[1]))
        relay.append(remote(b_far.at[high], bre.at[1], bz_s.at[1], bz_r.at[1], at_z[-1]))
        for r in (1, 3):
            from_bz.append(
                remote(b1.at[:, ring(z, r, NZ)], b2.at[r], bl_s.at[3 + r], bl_r.at[3 + r], at_z[r])
            )
        b2[0] = b1[:, z]

    def do_relay():
        for i, (part_of, who) in enumerate(((low, at_z[1]), (high, at_z[-1]))):
            relay[i].wait_recv()
            from_bz.append(
                remote(bre.at[i], b2.at[2, part_of], bz_s.at[2 + i], bz_r.at[2 + i], who)
            )

    def do_moved():
        for j in range(MB):
            for p in range(NP):
                rows = recv_a[p][sec[s * MB + j] >> 3]
                for h in range(2):
                    moved_v[j, :, h * H + p * HP : h * H + (p + 1) * HP] = rows[h]

    steps = dict(
        near=do_near, row=do_row, onz=do_onz, ony=do_ony, project=do_project,
        finish=do_finish, blocks=do_blocks, relay=do_relay, moved=do_moved,
        scaled=do_scaled,
    )
    for name, *which in GATHER:
        if (name == "near" or (name == "row" and which[0] == 0)) and which[-2] == 1:
            if which[-1] in core_n:
                core_n.pop(which[-1]).wait_recv()
        with jax.named_scope("_".join([name] + [str(w) for w in which])):
            steps[name](*which)
    back = [zf, zb, za, z]
    keys, values = kf[...].reshape(512, HD), vf[...].reshape(512, HD)
    line = lax.broadcasted_iota(jnp.int32, (128, 512), 0)
    token = ((line >> 5) << 7) + (line & 31)
    col = lax.broadcasted_iota(jnp.int32, (128, 512), 1)
    from_att = {}

    def do_attend(m):
        scores = lax.dot_general(
            qf[:, back[m]].reshape(128, HD), keys,
            (((1,), (1,)), ((), ())), preferred_element_type=F32,
        ) * ((D / 32) ** (-0.5))
        capped = 50.0 * jnp.tanh(scores / 50.0)
        expd = jnp.where(col <= token + back[m] * 32, jnp.exp(capped), 0.0)
        total = jnp.sum(expd, axis=-1, keepdims=True)
        numer = jnp.dot(expd.astype(BF16), values, preferred_element_type=F32)
        zz = back[m]
        at2[c, zz] = (numer / total).astype(BF16)
        from_att[m] = remote(
            at2.at[c, zz], at2.at[c, zz], cc_s.at[12 + zz], cc_r.at[12 + zz], at_c
        )

    do_attend(0)

    y_far, y_own, y_mid, z_side, z_far, z_own, z_mid, late = {}, {}, {}, {}, {}, {}, {}, {}

    def cols(p):
        return pl.ds(p * HP, HP)

    def mine_at(yy, q, i, p):
        return pbuf.at[yy, back[q], half[i], :, cols(p)]

    def do_part(q):
        if q == 0:
            load_wo.wait()
            w_o.wait_recv()
        from_att[q].wait_recv()
        res = jnp.dot(at2[0, back[q]], wobuf[0], preferred_element_type=F32)
        res = res + jnp.dot(at2[1, back[q]], wobuf[1], preferred_element_type=F32)
        pbuf[:, back[q]] = res.astype(BF16).reshape(NY, 2, ROWS, H)

    def do_far(q, i, p):
        y_far[q, i, p] = remote(
            mine_at(yf, q, i, p), yrh.at[q, i, :, cols(p)],
            dy_s.at[q, i, 0, p], dy_r.at[q, i, 0, p], (to_ya, to_yb)[i],
        )

    def do_own(q, i, p):
        source = mine_at((yb, ya)[i], q, i, p)
        if q == 3:
            z_side[1, i, p].wait_recv()
            z_side[2, i, p].wait_recv()
            total = source[...].astype(F32) + zrs[0, i, :, cols(p)].astype(F32)
            source[...] = (total + zrs[1, i, :, cols(p)].astype(F32)).astype(BF16)
        y_own[q, i, p] = remote(
            source, yro.at[q, i, :, cols(p)],
            dy_s.at[q, i, 1, p], dy_r.at[q, i, 1, p], (to_yb, to_ya)[i],
        )

    def do_side(q, i, p):
        z_side[q, i, p] = remote(
            mine_at((yb, ya)[i], q, i, p), zrs.at[q - 1, i, :, cols(p)],
            dx_s.at[q - 1, i, p], dx_r.at[q - 1, i, p], (to_zb, to_za)[q - 1],
        )

    def do_middle(q, i, p):
        y_far[q, i, p].wait_recv()
        source = mine_at((ya, yb)[i], q, i, p)
        total = source[...].astype(F32) + yrh[q, i, :, cols(p)].astype(F32)
        source[...] = total.astype(BF16)
        y_mid[q, i, p] = remote(
            source, yrm.at[q, i, :, cols(p)],
            dy_s.at[q, i, 2, p], dy_r.at[q, i, 2, p], (to_ya, to_yb)[i],
        )

    def reduced(q, i, p):
        total = mine_at(y, q, i, p)[...].astype(F32)
        if q == 0 or q == 3:
            y_own[q, i, p].wait_recv()
            total = total + yro[q, i, :, cols(p)].astype(F32)
        y_mid[q, i, p].wait_recv()
        return total + yrm[q, i, :, cols(p)].astype(F32)

    def send_z(value, kind, i, p, into, who):
        zs[kind, i, :, cols(p)] = value.astype(BF16)
        return remote(
            zs.at[kind, i, :, cols(p)], into.at[i, :, cols(p)],
            dz_s.at[kind, i, p], dz_r.at[kind, i, p], who,
        )

    def do_zfar(i, p):
        z_far[i, p] = send_z(reduced(0, i, p), 0, i, p, zrh, (to_za, to_zb)[i])

    def do_zown(i, p):
        z_own[i, p] = send_z(reduced(1 + i, i, p), 1, i, p, zro, (to_zb, to_za)[i])

    def do_zmid(i, p):
        total = reduced(2 - i, i, p)
        z_far[i, p].wait_recv()
        total = total + zrh[i, :, cols(p)].astype(F32)
        z_mid[i, p] = send_z(total, 2, i, p, zrm, (to_za, to_zb)[i])

    def do_cores():
        for copy in from_bz + from_lz:
            copy.wait_recv()
        late["blocks"] = remote(b2.at[:, :, o], b3, bl_s.at[7], bl_r.at[7], at_c)
        lfin[...] = lsum[...] + lrz[1] + lrz[2] + lrz[3]
        late["loss"] = remote(lfin, lrc, bl_s.at[15], bl_r.at[15], at_c)

    def do_place():
        late["loss"].wait_recv()
        late["blocks"].wait_recv()
        factor = 32.0 / (lfin[...] + lrc[...])[0, 0]

        def place(b, carry):
            source = blk[d * BLK + b] >> 5
            ry = (y - (source >> 3)) & 3
            rz = (z - ((source >> 1) & 3)) & 3
            mine = b2[rz, ry, c].astype(F32)
            theirs = b3[rz, ry].astype(F32)
            newacc_v[b] = jnp.where((source & 1) == c, mine, theirs) * factor
            return carry

        lax.fori_loop(0, BLK, place, 0)

    def do_finish_sum(i, p):
        total = reduced(3, i, p)
        z_own[i, p].wait_recv()
        z_mid[i, p].wait_recv()
        total = total + zro[i, :, cols(p)].astype(F32)
        fb[i, :, cols(p)] = total + zrm[i, :, cols(p)].astype(F32)
        if i == 1:
            late[p] = remote(
                fb.at[1, :, cols(p)], finr.at[:, cols(p)], df_s.at[p], df_r.at[p], at_c
            )

    steps = dict(
        part=do_part, far=do_far, own=do_own, side=do_side, middle=do_middle, zfar=do_zfar,
        zown=do_zown, zmid=do_zmid, cores=do_cores, place=do_place, finish=do_finish_sum,
        attend=do_attend,
    )
    for name, *which in REDUCE:
        with jax.named_scope("_".join([name] + [str(w) for w in which])):
            steps[name](*which)
    checked = [recv_a[p][sec[s * MB] >> 3].astype(F32) for p in range(NP)]
    for p in range(NP):
        late[p].wait_recv()
    mine = fb[0]
    theirs = finr[...]
    meansq = jnp.sum(mine * mine, axis=-1, keepdims=True)
    meansq = (meansq + jnp.sum(theirs * theirs, axis=-1, keepdims=True)) / D
    scale = lax.rsqrt(meansq + EPS)
    outb[c] = mine
    outb[o] = theirs
    for h in range(2):
        for p in range(NP):
            cols_of = slice(h * H + p * HP, h * H + (p + 1) * HP)
            change = outb[h, :, p * HP : (p + 1) * HP] * scale * gpost[:, cols_of]
            checkb[:, cols_of] = (checked[p][h] + change).astype(BF16)
    for copy in pending:
        copy.wait_send()


def put_out(moved, newacc, check, moved_hbm, newacc_hbm, check_hbm, sem):
    copies = [
        pltpu.make_async_copy(source, into, sem.at[i])
        for i, (source, into) in enumerate(
            ((newacc, newacc_hbm), (moved, moved_hbm), (check, check_hbm))
        )
    ]
    for copy in copies:
        copy.start()
    for copy in copies:
        copy.wait()


def on_device(act, sec, acc, blk, loss, gpre, wq, wkv, wo, gpost):
    tab = jnp.asarray(rotary_tables())
    any_ = pl.BlockSpec(memory_space=pl.ANY)
    vmem = pl.BlockSpec(memory_space=pltpu.VMEM)
    V = pltpu.VMEM
    dma = pltpu.SemaphoreType.DMA
    moved, newacc, check = pl.pallas_call(
        kernel,
        out_shape=(
            V((MB, ROWS, D), BF16),
            V((BLK, 2, D), F32),
            V((ROWS, D), BF16),
        ),
        in_specs=[pl.BlockSpec(memory_space=pltpu.HBM)] * 11,
        out_specs=(vmem, vmem, vmem),
        scratch_shapes=[
            V((MB, ROWS, D), BF16), V((NS, NP, 2, ROWS, HP), BF16),
            V((NS, 2, ROWS, HP), BF16), V((NS, 2, ROWS, HP), BF16),
            V((BLK, 2, D), F32),
            V((NY, NZ, 2, 2, D), BF16), V((NY, NZ, 2, 2, D), BF16),
            V((NZ, NY, 2, 2, D), BF16), V((NZ, NY, 2, D), BF16), V((2, 2, 2, 2, D), BF16),
            V((1, HD), F32), V((4, 1, HD), F32), V((1, HD), F32), V((4, 1, HD), F32),
            V((1, HD), F32), V((1, HD), F32),
            V((2, ROWS, HW), BF16), V((NY, NZ, 2, ROWS, HW), BF16), V((H, 4 * HD), BF16),
            V((2, HD, H), BF16), V((4, 4, 128, HD), F32), V((4, 128, HD), F32),
            V((4, 2, 128, HD), F32), V((NY, NZ, 32, HD), BF16), V((NY, NZ, 32, HD), BF16),
            V((NY, NZ, 32, HD), BF16), V((2, 4, 128, HD), BF16),
            V((NY, NZ, 2, ROWS, H), BF16), V((4, 2, ROWS, H), BF16), V((4, 2, ROWS, H), BF16),
            V((4, 2, ROWS, H), BF16), V((2, ROWS, H), BF16), V((2, ROWS, H), BF16),
            V((2, ROWS, H), BF16), V((3, 2, ROWS, H), BF16), V((2, ROWS, H), F32),
            V((ROWS, H), F32), V((2, ROWS, H), F32),
            V((2, NY, NZ, 32, HD), F32), pltpu.SMEM((64,), jnp.int32),
            pltpu.SMEM((1024,), jnp.int32), V((1, 1), F32), V((1, D), F32), V((1, D), F32),
            V((2, 2, ROWS, H), BF16),
            dma((15,)), dma((2 * NP,)), dma((2 * NP,)), dma((2, 2, NP)), dma((2, 2, NP)), dma((NS, NP)), dma((NS, NP)), dma((16,)), dma((16,)), dma((2, 3, NP)), dma((2, 3, NP)),
            dma((4, 2, 3, NP)), dma((4, 2, 3, NP)), dma((17,)), dma((17,)),
            dma((4, 2, 3, NP)), dma((4, 2, 3, NP)), dma((3, 2, NP)), dma((3, 2, NP)), dma((4,)), dma((4,)),
        ],
        compiler_params=pltpu.CompilerParams(
            collective_id=0, has_side_effects=True, vmem_limit_bytes=61 * 1024 * 1024
        ),
        name="restore",
    )(sec, blk, act, acc, loss, gpre, wq[0], wkv[0], wo[0], gpost, tab)
    moved, newacc, check = pl.pallas_call(
        put_out,
        out_shape=(
            jax.ShapeDtypeStruct((MB, ROWS, D), BF16),
            jax.ShapeDtypeStruct((BLK, 2, D), F32),
            jax.ShapeDtypeStruct((ROWS, D), BF16),
        ),
        in_specs=[vmem] * 3,
        out_specs=(any_, any_, any_),
        scratch_shapes=[dma((3,))],
        compiler_params=pltpu.CompilerParams(vmem_limit_bytes=8 * 1024 * 1024),
        name="put_out",
    )(moved, newacc, check)
    return moved, newacc, check[None]


def solution(mesh):
    placed = (
        P("section", "dp", None),
        P(),
        P("dp", "section", None),
        P(),
        P("section", "dp"),
        P("section", None),
        P("section", None, "dp"),
        P("section", None, "dp"),
        P("section", "dp", None),
        P("section", None),
    )
    return jax.shard_map(
        on_device,
        mesh=mesh,
        in_specs=placed,
        out_specs=(P("section", "dp", None), P("dp", "section", None), P("section", "dp", None)),
        check_vma=False,
    )
```
